128 devices in a mesh: rep: 1, seq: 128 (over z, y, x, core).
Axes of the slice: x: 4, y: 4, z: 4, core: 2. Of those that a mesh axis runs over, the one named last changes fastest.
Arguments:
- hidden: bfloat16 [16, 8192], P('rep')
- w_query: bfloat16 [8192, 8192], replicated
- w_key: bfloat16 [8192, 1024], replicated
- w_value: bfloat16 [8192, 1024], replicated
- w_out: bfloat16 [8192, 8192], P('seq')
- k_cache: bfloat16 [16, 8192, 8, 128], P('rep', 'seq')
- v_cache: bfloat16 [16, 8192, 8, 128], P('rep', 'seq')
- positions: int32 [16], P('rep')
Outputs:
- output 1: bfloat16 [16, 8192], P('rep')
- output 2: bfloat16 [16, 8192, 8, 128], P('rep', 'seq')
- output 3: bfloat16 [16, 8192, 8, 128], P('rep', 'seq')
All inputs are finite; a program needn't handle non-finite values.
Results may differ from the reference program's by a relative error of at most 0.0046317.
Values are sent between devices in bfloat16 or wider.
A program may use at most 1 GiB of HBM per device.

```python
import math
import jax
import jax.numpy as jnp
from jax import lax

D_MODEL = 8192
NUM_HEADS = 64
KV_HEADS = 8
HEAD_DIM = 128
BATCH_SIZE = 16
LOCAL_LEN = 64
SEQ_LEN = 8192


def query_shift(hidden, w_query):
    group_size = NUM_HEADS // KV_HEADS
    q_flat = jnp.dot(hidden, w_query, preferred_element_type=jnp.float32).astype(jnp.bfloat16).astype(jnp.float32)
    q_heads = q_flat.reshape(BATCH_SIZE, KV_HEADS, group_size, HEAD_DIM)
    gram_mat = jnp.einsum('bkgd,bkhd->bkgh', q_heads, q_heads)
    coeffs = jnp.linalg.solve(gram_mat, jnp.ones((BATCH_SIZE, KV_HEADS, group_size, 1), jnp.float32))
    score_drop = math.log(SEQ_LEN) - 1.0
    return -score_drop * HEAD_DIM ** 0.5 * jnp.einsum('bkgo,bkgd->bkd', coeffs, q_heads)


def setup_inputs(seed: int = 0, part: int = 0) -> dict:
    root = jax.random.key(seed)
    shared = jax.random.split(root, 4)
    part_keys = jax.random.split(jax.random.fold_in(root, part), 6)
    blocks = SEQ_LEN // LOCAL_LEN
    block_shape = (BATCH_SIZE, blocks, LOCAL_LEN, KV_HEADS, HEAD_DIM)
    cache_shape = (BATCH_SIZE, SEQ_LEN, KV_HEADS, HEAD_DIM)
    q_width = NUM_HEADS * HEAD_DIM
    kv_width = KV_HEADS * HEAD_DIM
    hidden = jax.random.normal(part_keys[0], (BATCH_SIZE, D_MODEL), jnp.float32).astype(jnp.bfloat16)
    w_query = (jax.random.normal(shared[0], (D_MODEL, q_width), jnp.float32) * D_MODEL ** -0.5).astype(jnp.bfloat16)
    w_key = (jax.random.normal(shared[1], (D_MODEL, kv_width), jnp.float32) * D_MODEL ** -0.5).astype(jnp.bfloat16)
    w_value = (jax.random.normal(shared[2], (D_MODEL, kv_width), jnp.float32) * D_MODEL ** -0.5).astype(jnp.bfloat16)
    w_out = (jax.random.normal(shared[3], (q_width, D_MODEL), jnp.float32) * q_width ** -0.5).astype(jnp.bfloat16)
    key_scale = jax.random.uniform(part_keys[1], (BATCH_SIZE, blocks, 1, KV_HEADS, 1), jnp.float32, 0.5, 1.5)
    key_noise = jax.random.normal(part_keys[2], block_shape, jnp.float32) * key_scale
    k_cache = key_noise.reshape(cache_shape) + query_shift(hidden, w_query)[:, None]
    v_base = jax.random.normal(part_keys[3], (BATCH_SIZE, blocks, 1, KV_HEADS, HEAD_DIM), jnp.float32)
    v_cache = (v_base + jax.random.normal(part_keys[4], block_shape, jnp.float32)).reshape(cache_shape)
    positions = jax.random.randint(part_keys[5], (BATCH_SIZE,), SEQ_LEN // 4, SEQ_LEN, dtype=jnp.int32)
    return {'hidden': hidden, 'w_query': w_query, 'w_key': w_key, 'w_value': w_value, 'w_out': w_out, 'k_cache': k_cache.astype(jnp.bfloat16), 'v_cache': v_cache.astype(jnp.bfloat16), 'positions': positions}


def reference(hidden, w_query, w_key, w_value, w_out, k_cache, v_cache, positions):
    group_size = NUM_HEADS // KV_HEADS
    q_flat = jnp.dot(hidden, w_query, preferred_element_type=jnp.float32).astype(jnp.bfloat16)
    key_new = jnp.dot(hidden, w_key, preferred_element_type=jnp.float32).astype(jnp.bfloat16).reshape(BATCH_SIZE, KV_HEADS, HEAD_DIM)
    value_new = jnp.dot(hidden, w_value, preferred_element_type=jnp.float32).astype(jnp.bfloat16).reshape(BATCH_SIZE, KV_HEADS, HEAD_DIM)
    seq_ids = jnp.arange(SEQ_LEN)
    at_pos = (seq_ids[None, :] == positions[:, None])[:, :, None, None]
    k_updated = jnp.where(at_pos, key_new[:, None], k_cache)
    v_updated = jnp.where(at_pos, value_new[:, None], v_cache)
    is_valid = seq_ids[None, :] <= positions[:, None]
    q_heads = q_flat.astype(jnp.float32).reshape(BATCH_SIZE, KV_HEADS, group_size, HEAD_DIM)

    def one_row(row_args):
        q_row, k_row, v_row, valid_row = row_args
        scores = jnp.einsum('kgd,skd->kgs', q_row, k_row.astype(jnp.float32)) * HEAD_DIM ** -0.5
        scores = jnp.where(valid_row[None, None, :], scores, -jnp.inf)
        weights = jax.nn.softmax(scores, axis=-1)
        return jnp.einsum('kgs,skd->kgd', weights, v_row.astype(jnp.float32))

    attended = lax.map(one_row, (q_heads, k_updated, v_updated, is_valid))
    combined = attended.reshape(BATCH_SIZE, NUM_HEADS * HEAD_DIM).astype(jnp.bfloat16)
    result = jnp.dot(combined, w_out, preferred_element_type=jnp.float32).astype(jnp.bfloat16)
    return result, k_updated, v_updated
```

```python
import functools
import jax
import jax.numpy as jnp
from jax import lax
from jax.experimental import pallas as pl
from jax.experimental.pallas import tpu as pltpu
from jax.sharding import PartitionSpec as P

BF16 = jnp.bfloat16
F32 = jnp.float32
MESH = pl.DeviceIdType.MESH
KCH = 8
RING = (0, 1, 2, 1)


def offsets():
    offs = [(dz, dy, dx) for dz in range(4) for dy in range(4) for dx in range(4)][1:]
    return sorted(offs, key=lambda o: -(RING[o[0]] + RING[o[1]] + RING[o[2]]))


def main_kernel(pos_ref, x_ref, wq_ref, wk_ref, wv_ref, wo_ref, k_ref, v_ref,
                y_ref, kvnew_ref,
                wqb, wkvb, kbuf, vbuf, wob, qsend, qrecv, kvsend, kvrecv, kvf, qf, colidx,
                osend, orecv, ssend, srecv, ysend, yrecv, yb, yg,
                wsem, ksem, d2d_send, d2d_recv, q_send, q_recv, o_send, o_recv,
                s_send, s_recv, ys_send, ys_recv, yg_send, yg_recv, pp_send, pp_recv):
    me = lax.axis_index("seq")
    chip, core = me // 2, me % 2
    cx, cy, cz = chip % 4, (chip // 4) % 4, chip // 16
    other = 1 - core
    cube = (cz % 2) * 4 + (cy % 2) * 2 + (cx % 2)
    bz, by, bx = cz - cz % 2, cy - cy % 2, cx - cx % 2
    slot = cube * 2 + core

    def dev(d):
        return {"seq": d}

    def chip_at(o):
        return ((cz + o[0]) % 4) * 16 + ((cy + o[1]) % 4) * 4 + (cx + o[2]) % 4

    def cube_chip(o):
        t = (cube + o) % 8
        return (bz + t // 4) * 16 + (by + (t // 2) % 2) * 4 + bx + t % 2

    rows = 8192 // KCH
    qcol = pl.multiple_of(slot * 512, 512)
    kcol = pl.multiple_of(cube * 128, 128)

    def wq_copy(i):
        return pltpu.make_async_copy(wq_ref.at[pl.ds(i * rows, rows), pl.ds(qcol, 512)],
                                     wqb.at[pl.ds(i * rows, rows)], wsem.at[i])

    def wkv_copy(ref, i):
        return pltpu.make_async_copy(ref.at[pl.ds(i * rows, rows), pl.ds(kcol, 128)],
                                     wkvb.at[pl.ds(i * rows, rows)], wsem.at[KCH + i])

    for i in range(KCH):
        wq_copy(i).start()

    @pl.when(core == 0)
    def _():
        for i in range(KCH):
            wkv_copy(wk_ref, i).start()

    @pl.when(core == 1)
    def _():
        for i in range(KCH):
            wkv_copy(wv_ref, i).start()

    mine = pl.multiple_of(core * 8, 8)
    theirs = pl.multiple_of(other * 8, 8)
    loc = [pltpu.make_async_copy(k_ref.at[pl.ds(mine, 8)], kbuf.at[:, core], ksem.at[0]),
           pltpu.make_async_copy(v_ref.at[pl.ds(mine, 8)], vbuf.at[:, core], ksem.at[1]),
           pltpu.make_async_copy(wo_ref, wob.at[core], ksem.at[2])]
    for c in loc:
        c.start()

    bar = pltpu.get_barrier_semaphore()
    partner = chip * 2 + other
    for o in offsets():
        pl.semaphore_signal(bar, inc=1, device_id=dev(chip_at(o) * 2 + core), device_id_type=MESH)
    for o in range(8):
        pl.semaphore_signal(bar, inc=1, device_id=dev(cube_chip(o) * 2 + other), device_id_type=MESH)

    col = lax.broadcasted_iota(jnp.int32, (64, 1024), 1)
    row = lax.broadcasted_iota(jnp.int32, (64, 1024), 0)
    colidx[...] = jnp.where(col % 8 == row // 8, chip * 128 + col // 8, 1 << 30)

    accq = jnp.zeros((16, 512), F32)
    for i in range(KCH):
        wq_copy(i).wait()
        accq = accq + jnp.dot(x_ref[:, i * rows:(i + 1) * rows], wqb[i * rows:(i + 1) * rows, :],
                              preferred_element_type=F32)
    for h in range(2):
        qsend[h] = accq[h * 8:h * 8 + 8].astype(BF16)
    acck = jnp.zeros((16, 128), F32)
    for i in range(KCH):
        wkv_copy(wk_ref, i).wait()
        acck = acck + jnp.dot(x_ref[:, i * rows:(i + 1) * rows], wkvb[i * rows:(i + 1) * rows, :],
                              preferred_element_type=F32)
    for h in range(2):
        kvsend[h] = acck[h * 8:h * 8 + 8].astype(BF16)
    pl.semaphore_wait(bar, 71)

    def rcopy(src, dst, ss, rs, d):
        return pltpu.make_async_remote_copy(src_ref=src, dst_ref=dst, send_sem=ss, recv_sem=rs,
                                            device_id=dev(d), device_id_type=MESH)

    targets = [(cube_chip(o), 0) for o in (7, 6, 5, 3, 4, 2, 1)]
    for ch, _ in targets:
        for c2 in (core, other):
            rcopy(qsend.at[c2], qrecv.at[slot], q_send.at[0], q_recv.at[0], ch * 2 + c2).start()
    rcopy(qsend.at[other], qrecv.at[slot], q_send.at[0], q_recv.at[0], partner).start()
    for ch, _ in targets:
        for c2 in (core, other):
            rcopy(kvsend, kvrecv.at[core * 8 + cube], q_send.at[1], q_recv.at[1], ch * 2 + c2).start()
    rcopy(kvsend, kvrecv.at[core * 8 + cube], q_send.at[1], q_recv.at[1], partner).start()
    dd = [rcopy(k_ref.at[pl.ds(theirs, 8)], kbuf.at[:, core], d2d_send.at[0], d2d_recv.at[0], partner),
          rcopy(v_ref.at[pl.ds(theirs, 8)], vbuf.at[:, core], d2d_send.at[1], d2d_recv.at[1], partner),
          rcopy(wo_ref, wob.at[core], d2d_send.at[2], d2d_recv.at[2], partner)]
    for c in dd:
        c.start()
    qrecv[slot] = qsend[core]
    kvrecv[core * 8 + cube] = kvsend[...]

    def wait_all(ref, sem):
        pltpu.make_async_copy(ref, ref, sem).wait()

    wait_all(qrecv.at[pl.ds(0, 15)], q_recv.at[0])
    for s in range(16):
        q8 = qrecv[s].astype(F32)
        for j in range(4):
            qf[:, s * 4 + j, :] = q8[:, j * 128:(j + 1) * 128]
    wait_all(kvrecv.at[pl.ds(0, 15)], q_recv.at[1])
    for kv in range(2):
        for h in range(8):
            for half in range(2):
                kvf[kv, half, :, h, :] = kvrecv[kv * 8 + h, half].astype(F32)
    kvnew_ref[...] = kvf[...].astype(BF16)
    loc[0].wait()
    loc[1].wait()
    dd[0].wait_recv()
    dd[1].wait_recv()

    lane = lax.broadcasted_iota(jnp.int32, (64, 128), 1)
    stats = jnp.zeros((64, 128), F32)
    scale = 128 ** -0.5
    neg = -jnp.inf
    for b in range(8):
        pos = pos_ref[core * 8 + b]
        qb = qf[b]
        kn = jnp.broadcast_to(kvf[0, core, b][:, None, :], (8, 8, 128)).reshape(64, 128)
        vn = jnp.broadcast_to(kvf[1, core, b][:, None, :], (8, 8, 128)).reshape(64, 128)
        s = lax.dot_general(qb.astype(BF16), kbuf[b].reshape(1024, 128), (((1,), (1,)), ((), ())),
                            preferred_element_type=F32) * scale
        s = jnp.where(colidx[...] < pos, s, neg)
        snew = jnp.sum(qb * kn, axis=1, keepdims=True) * scale
        here = jnp.full((64, 1), pos // 128, jnp.int32) == chip
        snew = jnp.where(here, snew, neg)
        m = jnp.maximum(jnp.max(s, axis=1, keepdims=True), snew)
        msafe = jnp.where(m == neg, 0.0, m)
        p = jnp.exp(s - msafe)
        pn = jnp.exp(snew - msafe)
        l = jnp.sum(p, axis=1, keepdims=True) + pn
        o = jnp.dot(p.astype(BF16), vbuf[b].reshape(1024, 128), preferred_element_type=F32) + pn * vn
        osend[:, b, :] = o
        stats = jnp.where(lane == b, m, stats)
        stats = jnp.where(lane == 8 + b, l, stats)
    ssend[:, 0, :] = stats

    for o in offsets():
        d = chip_at(o)
        rcopy(osend.at[d], orecv.at[chip], o_send, o_recv, d * 2 + core).start()
        rcopy(ssend.at[d], srecv.at[chip], s_send, s_recv, d * 2 + core).start()
    orecv[chip] = osend[chip]
    srecv[chip] = ssend[chip]
    loc[2].wait()
    dd[2].wait_recv()
    wait_all(srecv.at[pl.ds(0, 63)], s_recv)
    st = jnp.concatenate([srecv[:, 0, :], jnp.zeros((64, 128), F32)], axis=0).T
    mt = st[0:8, 0:64]
    lt = st[8:16, 0:64]
    mx = jnp.max(mt, axis=1, keepdims=True)
    w = jnp.exp(mt - mx)
    tot = jnp.sum(w * lt, axis=1, keepdims=True)
    wait_all(orecv.at[pl.ds(0, 63)], o_recv)
    acc = jnp.zeros((8, 128), F32)
    for i in range(64):
        acc = acc + w[:, i:i + 1] * orecv[i]
    ob = (acc / tot).astype(BF16)

    for j in range(16):
        wj = wob[:, :, j * 512:(j + 1) * 512].reshape(128, 512)
        part = jnp.dot(ob, wj, preferred_element_type=F32)
        for jj in range(4):
            ysend[j * 4 + jj] = part[:, jj * 128:(jj + 1) * 128]
    for o in offsets():
        d = chip_at(o)
        rcopy(ysend.at[d], yrecv.at[chip], ys_send, ys_recv, d * 2 + core).start()
    yrecv[chip] = ysend[chip]
    wait_all(yrecv.at[pl.ds(0, 63)], ys_recv)
    acc = yrecv[0]
    for i in range(1, 64):
        acc = acc + yrecv[i]
    yb[...] = acc.astype(BF16)

    for o in offsets():
        rcopy(yb, yg.at[core, chip], yg_send, yg_recv, chip_at(o) * 2 + core).start()
    yg[core, chip] = yb[...]
    wait_all(yg.at[0, pl.ds(0, 63)], yg_recv)
    fwd = rcopy(yg.at[core], yg.at[core], pp_send, pp_recv, partner)
    fwd.start()
    y_ref[core] = yg[core]
    fwd.wait_recv()
    y_ref[other] = yg[other]

    fwd.wait_send()
    wait_all(yg.at[0, pl.ds(0, 63)], yg_send)
    wait_all(yrecv.at[pl.ds(0, 63)], ys_send)
    wait_all(orecv.at[pl.ds(0, 63)], o_send)
    wait_all(srecv.at[pl.ds(0, 63)], s_send)
    wait_all(qrecv.at[pl.ds(0, 15)], q_send.at[0])
    wait_all(kvrecv.at[pl.ds(0, 15)], q_send.at[1])
    for c in dd:
        c.wait_send()


def update_kernel(pos_ref, new_ref, k_ref, v_ref, ko_ref, vo_ref, buf, isem, osem):
    me = lax.axis_index("seq")
    base = me * 64
    n = 8
    srcs, dsts = (k_ref, v_ref), (ko_ref, vo_ref)

    def rd(t, i):
        return pltpu.make_async_copy(srcs[t].at[pl.ds(i * 2, 2)], buf.at[t, pl.ds(i * 2, 2)], isem.at[t, i])

    def wr(t, i):
        return pltpu.make_async_copy(buf.at[t, pl.ds(i * 2, 2)], dsts[t].at[pl.ds(i * 2, 2)], osem.at[t, i])

    for i in range(n):
        for t in range(2):
            rd(t, i).start()
    for i in range(n):
        for t in range(2):
            rd(t, i).wait()
            for b in (2 * i, 2 * i + 1):
                r = pos_ref[b] - base

                @pl.when((r >= 0) & (r < 64))
                def _():
                    buf[t, b, r] = new_ref[t, b]
            wr(t, i).start()
    for i in range(n):
        for t in range(2):
            wr(t, i).wait()


def solution(mesh):
    cache_spec = P('rep', 'seq', None, None)
    in_specs = (P('rep', None), P(), P(), P(), P('seq', None), cache_spec, cache_spec, P('rep'))
    out_specs = (P('rep', None), cache_spec, cache_spec)
    vmem, anyspace, smem = (pl.BlockSpec(memory_space=s) for s in (pltpu.VMEM, pl.ANY, pltpu.SMEM))
    dma = pltpu.SemaphoreType.DMA

    def local_step(x, wq, wk, wv, wo, k, v, pos):
        y, new = pl.pallas_call(
            main_kernel,
            name="decode",
            out_shape=(jax.ShapeDtypeStruct((2, 64, 8, 128), BF16),
                       jax.ShapeDtypeStruct((2, 2, 8, 8, 128), BF16)),
            in_specs=[smem, vmem] + [anyspace] * 6,
            out_specs=(vmem, vmem),
            scratch_shapes=[
                pltpu.VMEM((8192, 512), BF16), pltpu.VMEM((8192, 128), BF16),
                pltpu.VMEM((8, 2, 512, 128), BF16), pltpu.VMEM((8, 2, 512, 128), BF16),
                pltpu.VMEM((2, 64, 8192), BF16),
                pltpu.VMEM((2, 8, 512), BF16), pltpu.VMEM((16, 8, 512), BF16),
                pltpu.VMEM((2, 8, 128), BF16), pltpu.VMEM((16, 2, 8, 128), BF16),
                pltpu.VMEM((2, 2, 8, 8, 128), F32), pltpu.VMEM((8, 64, 128), F32),
                pltpu.VMEM((64, 1024), jnp.int32),
                pltpu.VMEM((64, 8, 128), F32), pltpu.VMEM((64, 8, 128), F32),
                pltpu.VMEM((64, 1, 128), F32), pltpu.VMEM((64, 1, 128), F32),
                pltpu.VMEM((64, 8, 128), F32), pltpu.VMEM((64, 8, 128), F32),
                pltpu.VMEM((8, 128), BF16), pltpu.VMEM((2, 64, 8, 128), BF16),
                dma((2 * KCH,)), dma((3,)), dma((3,)), dma((3,)), dma((2,)), dma((2,)),
                dma, dma, dma, dma, dma, dma, dma, dma, dma, dma,
            ],
            compiler_params=pltpu.CompilerParams(collective_id=0, has_side_effects=True,
                                                 vmem_limit_bytes=60 << 20),
        )(pos, x, wq, wk, wv, wo, k.reshape(16, 512, 128), v.reshape(16, 512, 128))
        result = y.transpose(0, 2, 1, 3).reshape(16, 8192)
        ko, vo = pl.pallas_call(
            update_kernel,
            name="update",
            out_shape=(jax.ShapeDtypeStruct(k.shape, BF16),) * 2,
            in_specs=[smem, vmem, anyspace, anyspace],
            out_specs=(anyspace, anyspace),
            scratch_shapes=[pltpu.VMEM((2, 16, 64, 8, 128), BF16), dma((2, 8)), dma((2, 8))],
            compiler_params=pltpu.CompilerParams(vmem_limit_bytes=32 << 20),
        )(pos, new.reshape(2, 16, 8, 128), k, v)
        return result, ko, vo

    return jax.shard_map(local_step, mesh=mesh, in_specs=in_specs, out_specs=out_specs, check_vma=False)
```

```python
import functools
import jax
import jax.numpy as jnp
from jax import lax
from jax.experimental import pallas as pl
from jax.experimental.pallas import tpu as pltpu
from jax.sharding import PartitionSpec as P

BF16 = jnp.bfloat16
F32 = jnp.float32
MESH = pl.DeviceIdType.MESH
DECODE_VMEM = 40
KCH = 8
RING = (0, 1, 2, 1)


def offsets():
    offs = [(dz, dy, dx) for dz in range(4) for dy in range(4) for dx in range(4)][1:]
    return sorted(offs, key=lambda o: -(RING[o[0]] + RING[o[1]] + RING[o[2]]))


def hops(o):
    return RING[o[0]] + RING[o[1]] + RING[o[2]]


def colour_offsets():
    best = {}
    for o in sorted(offsets(), key=lambda o: (hops(o), o)):
        d = ((o[2] + o[0]) % 4, (o[1] + o[0]) % 4)
        neg = ((-d[0]) % 4, (-d[1]) % 4)
        if d == (0, 0) or d in best or (d == neg and any(c % 2 for c in o)):
            continue
        best[d] = o
        best[neg] = tuple(-c % 4 for c in o)
    return sorted(best.values(), key=lambda o: -hops(o))


NEAR = [z * 16 + y * 4 + x for z in range(4) for y in range(4) for x in range(4) if hops((z, y, x)) <= 1]


def start_distance(chip):
    ring = lambda c: jnp.where(c == 3, 1, c)
    return ring(chip % 4) + ring((chip // 4) % 4) + ring(chip // 16)


def main_kernel(pos_hbm, x_hbm, wq_ref, wk_ref, wv_ref, wo_ref, k_ref, v_ref,
                y_ref, kvnew_ref,
                pos_ref, x_ref, khalf, vhalf, wqb, wkvb, kbuf, vbuf, wob, qsend, qrecv, kvsend, kvrecv, kvf, qf, colidx,
                osend, orecv, ssend, srecv, ysend, yrecv, yb, yg,
                xsem, wsem, ksem, d2d_send, d2d_recv, q_send, q_recv, o_send, o_recv,
                s_send, s_recv, ys_send, ys_recv, yg_send, yg_recv, pp_send, pp_recv, pn_send, pn_recv):
    me = lax.axis_index("seq")
    chip, core = me // 2, me % 2
    cx, cy, cz = chip % 4, (chip // 4) % 4, chip // 16
    other = 1 - core
    colour = ((cx + cz) % 4) * 4 + (cy + cz) % 4
    slot = colour * 2 + core

    def dev(d):
        return {"seq": d}

    def chip_at(o):
        return ((cz + o[0]) % 4) * 16 + ((cy + o[1]) % 4) * 4 + (cx + o[2]) % 4

    rows = 8192 // KCH
    qcol = pl.multiple_of(slot * 256, 256)
    kcol = pl.multiple_of((colour % 8) * 128, 128)

    def wq_copy(i):
        return pltpu.make_async_copy(wq_ref.at[pl.ds(i * rows, rows), pl.ds(qcol, 256)],
                                     wqb.at[pl.ds(i * rows, rows)], wsem.at[i])

    def wkv_copy(ref, i):
        return pltpu.make_async_copy(ref.at[pl.ds(i * rows, rows), pl.ds(kcol, 128)],
                                     wkvb.at[pl.ds(i * rows, rows)], wsem.at[KCH + i])

    xload = [pltpu.make_async_copy(x_hbm, x_ref, xsem.at[0]),
             pltpu.make_async_copy(pos_hbm, pos_ref, xsem.at[1])]
    for c in xload:
        c.start()
    for i in range(KCH):
        wq_copy(i).start()

    for ref, cond in ((wk_ref, colour < 8), (wv_ref, colour >= 8)):
        @pl.when((core == 1) & cond)
        def _():
            for i in range(KCH):
                wkv_copy(ref, i).start()

    mine = pl.multiple_of(core * 8, 8)
    theirs = pl.multiple_of(other * 8, 8)
    loc = [pltpu.make_async_copy(k_ref.at[pl.ds(mine, 8)], kbuf.at[:, core], ksem.at[0]),
           pltpu.make_async_copy(v_ref.at[pl.ds(mine, 8)], vbuf.at[:, core], ksem.at[1]),
           pltpu.make_async_copy(wo_ref, wob.at[core], ksem.at[2]),
           pltpu.make_async_copy(k_ref.at[pl.ds(theirs, 8)], khalf, ksem.at[3]),
           pltpu.make_async_copy(v_ref.at[pl.ds(theirs, 8)], vhalf, ksem.at[4])]

    bar = pltpu.get_barrier_semaphore()
    partner = chip * 2 + other
    for o in offsets():
        pl.semaphore_signal(bar, inc=1, device_id=dev(chip_at(o) * 2 + core), device_id_type=MESH)
    for o in [(0, 0, 0)] + colour_offsets():
        pl.semaphore_signal(bar, inc=1, device_id=dev(chip_at(o) * 2 + other), device_id_type=MESH)
    near = start_distance(chip) <= 1

    @pl.when(near)
    def _():
        for d in range(64):
            pl.semaphore_signal(bar, inc=1, device_id=dev(d * 2 + other), device_id_type=MESH)

    col = lax.broadcasted_iota(jnp.int32, (64, 1024), 1)
    row = lax.broadcasted_iota(jnp.int32, (64, 1024), 0)
    colidx[...] = jnp.where(col % 8 == row // 8, chip * 128 + col // 8, 1 << 30)

    for c in xload:
        c.wait()
    accq = jnp.zeros((16, 256), F32)
    for i in range(KCH):
        wq_copy(i).wait()
        if i == KCH // 2:
            for t in (3, 4, 0, 1):
                loc[t].start()
        accq = accq + jnp.dot(x_ref[:, i * rows:(i + 1) * rows], wqb[i * rows:(i + 1) * rows, :],
                              preferred_element_type=F32)
    for h in range(2):
        qsend[h] = accq[h * 8:h * 8 + 8].astype(BF16)
    loc[2].start()
    pl.semaphore_wait(bar, 79 + len(NEAR))

    def rcopy(src, dst, ss, rs, d):
        return pltpu.make_async_remote_copy(src_ref=src, dst_ref=dst, send_sem=ss, recv_sem=rs,
                                            device_id=dev(d), device_id_type=MESH)

    near_chips = [chip_at(o) for o in colour_offsets()]
    for ch in near_chips:
        for c2 in (core, other):
            rcopy(qsend.at[c2], qrecv.at[slot], q_send.at[0], q_recv.at[0], ch * 2 + c2).start()
    rcopy(qsend.at[other], qrecv.at[slot], q_send.at[0], q_recv.at[0], partner).start()
    loc[3].wait()
    loc[4].wait()
    dk = [rcopy(khalf.at[b], kbuf.at[b, core], d2d_send.at[b], d2d_recv.at[b], partner) for b in range(8)]
    dv = [rcopy(vhalf.at[b], vbuf.at[b, core], d2d_send.at[8 + b], d2d_recv.at[8 + b], partner) for b in range(8)]
    dw = rcopy(wo_ref, wob.at[core], d2d_send.at[16], d2d_recv.at[16], partner)
    dd = [c for pair in zip(dk, dv) for c in pair] + [dw]
    for c in dd:
        c.start()
    qrecv[slot] = qsend[core]

    @pl.when(core == 1)
    def _():
        acck = jnp.zeros((16, 128), F32)
        for i in range(KCH):
            wkv_copy(wk_ref, i).wait()
            acck = acck + jnp.dot(x_ref[:, i * rows:(i + 1) * rows], wkvb[i * rows:(i + 1) * rows, :],
                                  preferred_element_type=F32)
        for h in range(2):
            kvsend[h] = acck[h * 8:h * 8 + 8].astype(BF16)
        for ch in near_chips:
            for c2 in (core, other):
                rcopy(kvsend, kvrecv.at[colour], q_send.at[1], q_recv.at[1], ch * 2 + c2).start()
        rcopy(kvsend, kvrecv.at[colour], q_send.at[1], q_recv.at[1], partner).start()
        kvrecv[colour] = kvsend[...]

    def wait_all(ref, sem):
        pltpu.make_async_copy(ref, ref, sem).wait()

    wait_all(qrecv.at[pl.ds(0, 31)], q_recv.at[0])
    for s in range(32):
        q8 = qrecv[s].astype(F32)
        for j in range(2):
            qf[:, s * 2 + j, :] = q8[:, j * 128:(j + 1) * 128]

    @pl.when(core == 0)
    def _():
        wait_all(kvrecv.at[pl.ds(0, 16)], q_recv.at[1])

    @pl.when(core == 1)
    def _():
        wait_all(kvrecv.at[pl.ds(0, 15)], q_recv.at[1])

    for kv in range(2):
        for h in range(8):
            for half in range(2):
                kvf[kv, half, :, h, :] = kvrecv[kv * 8 + h, half].astype(F32)
    kvnew_ref[...] = kvf[...].astype(BF16)
    loc[0].wait()
    loc[1].wait()

    lane = lax.broadcasted_iota(jnp.int32, (64, 128), 1)
    stats = jnp.zeros((64, 128), F32)
    scale = 128 ** -0.5
    neg = -jnp.inf
    for b in range(8):
        pos = pos_ref[core * 8 + b]
        qb = qf[b]
        kn = jnp.broadcast_to(kvf[0, core, b][:, None, :], (8, 8, 128)).reshape(64, 128)
        vn = jnp.broadcast_to(kvf[1, core, b][:, None, :], (8, 8, 128)).reshape(64, 128)
        dk[b].wait_recv()
        s = lax.dot_general(qb.astype(BF16), kbuf[b].reshape(1024, 128), (((1,), (1,)), ((), ())),
                            preferred_element_type=F32) * scale
        s = jnp.where(colidx[...] < pos, s, neg)
        snew = jnp.sum(qb * kn, axis=1, keepdims=True) * scale
        here = jnp.full((64, 1), pos // 128, jnp.int32) == chip
        snew = jnp.where(here, snew, neg)
        m = jnp.maximum(jnp.max(s, axis=1, keepdims=True), snew)
        msafe = jnp.where(m == neg, 0.0, m)
        p = jnp.exp(s - msafe)
        pn = jnp.exp(snew - msafe)
        l = jnp.sum(p, axis=1, keepdims=True) + pn
        dv[b].wait_recv()
        o = jnp.dot(p.astype(BF16), vbuf[b].reshape(1024, 128), preferred_element_type=F32) + pn * vn
        osend[:, b, :] = o
        stats = jnp.where(lane == b, m, stats)
        stats = jnp.where(lane == 8 + b, l, stats)
    ssend[:, 0, :] = stats

    for o in offsets():
        d = chip_at(o)
        rcopy(osend.at[d], orecv.at[chip], o_send, o_recv, d * 2 + core).start()
        rcopy(ssend.at[d], srecv.at[chip], s_send, s_recv, d * 2 + core).start()
    orecv[chip] = osend[chip]
    srecv[chip] = ssend[chip]
    loc[2].wait()
    dw.wait_recv()
    wait_all(srecv.at[pl.ds(0, 63)], s_recv)
    st = jnp.concatenate([srecv[:, 0, :], jnp.zeros((64, 128), F32)], axis=0).T
    mt = st[0:8, 0:64]
    lt = st[8:16, 0:64]
    mx = jnp.max(mt, axis=1, keepdims=True)
    w = jnp.exp(mt - mx)
    tot = jnp.sum(w * lt, axis=1, keepdims=True)
    wait_all(orecv.at[pl.ds(0, 63)], o_recv)
    acc = jnp.zeros((8, 128), F32)
    for i in range(64):
        acc = acc + w[:, i:i + 1] * orecv[i]
    ob = (acc / tot).astype(BF16)

    pending = []
    for dz, dy in sorted([(a, b) for a in range(4) for b in range(4)], key=lambda o: -(RING[o[0]] + RING[o[1]])):
        r = ((cz + dz) % 4) * 4 + (cy + dy) % 4
        wj = wob[:, :, pl.ds(pl.multiple_of(r * 512, 512), 512)].reshape(128, 512)
        part = jnp.dot(ob, wj, preferred_element_type=F32)
        for jj in range(4):
            ysend[r * 4 + jj] = part[:, jj * 128:(jj + 1) * 128]
        for d in pending:
            rcopy(ysend.at[d], yrecv.at[chip], ys_send, ys_recv, d * 2 + core).start()
        pending = [chip_at((dz, dy, dx)) for dx in (2, 1, 3, 0) if (dz, dy, dx) != (0, 0, 0)]
    for d in pending:
        rcopy(ysend.at[d], yrecv.at[chip], ys_send, ys_recv, d * 2 + core).start()
    yrecv[chip] = ysend[chip]
    wait_all(yrecv.at[pl.ds(0, 63)], ys_recv)
    acc = yrecv[0]
    for i in range(1, 64):
        acc = acc + yrecv[i]
    yb[...] = acc.astype(BF16)

    for o in offsets():
        rcopy(yb, yg.at[core, chip], yg_send, yg_recv, chip_at(o) * 2 + core).start()
    for t in NEAR:
        rcopy(yb, yg.at[core, chip], pn_send, pn_recv, t * 2 + other).start()
    yg[core, chip] = yb[...]
    wait_all(yg.at[0, pl.ds(0, 63)], yg_recv)
    fwd = rcopy(yg.at[core], yg.at[core], pp_send, pp_recv, partner)

    @pl.when(near)
    def _():
        wait_all(yg.at[0], pn_recv)

    @pl.when(jnp.logical_not(near))
    def _():
        fwd.start()
        fwd.wait_recv()
        fwd.wait_send()

    out = pltpu.make_async_copy(yg, y_ref, ksem.at[0])
    out.start()

    wait_all(yg.at[0, pl.ds(0, 63)], yg_send)
    wait_all(yg.at[0, pl.ds(0, len(NEAR))], pn_send)
    wait_all(yrecv.at[pl.ds(0, 63)], ys_send)
    wait_all(orecv.at[pl.ds(0, 63)], o_send)
    wait_all(srecv.at[pl.ds(0, 63)], s_send)
    wait_all(qrecv.at[pl.ds(0, 31)], q_send.at[0])

    @pl.when(core == 1)
    def _():
        wait_all(kvrecv.at[pl.ds(0, 16)], q_send.at[1])
        wait_all(kvrecv.at[pl.ds(0, 15)], q_send.at[1])

    for c in dd:
        c.wait_send()
    out.wait()


EARLY = 3


def reads_and_writes(srcs, dsts, buf, isem, osem):
    rd = lambda t, i: pltpu.make_async_copy(srcs[t].at[pl.ds(i * 2, 2)], buf.at[t, pl.ds(i * 2, 2)], isem.at[t, i])
    wr = lambda t, i: pltpu.make_async_copy(buf.at[t, pl.ds(i * 2, 2)], dsts[t].at[pl.ds(i * 2, 2)], osem.at[t, i])
    return rd, wr


def copy_kernel(k_ref, v_ref, ko_ref, vo_ref, buf, isem, osem):
    chip = lax.axis_index("seq") // 2
    rd, wr = reads_and_writes((k_ref, v_ref), (ko_ref, vo_ref), buf, isem, osem)
    order = [(t, i) for i in range(8) for t in range(2)]

    @pl.when(start_distance(chip) <= EARLY)
    def _():
        for t, i in order:
            rd(t, i).start()
        for t, i in order:
            rd(t, i).wait()
            wr(t, i).start()
        for t, i in order:
            wr(t, i).wait()


def update_kernel(pos_ref, new_ref, y_ref, k_ref, v_ref, km_ref, vm_ref, yo_ref, ko_ref, vo_ref,
                  buf, ysem, isem, osem, rsem):
    me = lax.axis_index("seq")
    base = me * 64
    early = start_distance(me // 2) <= EARLY
    yout = pltpu.make_async_copy(y_ref, yo_ref, ysem)
    yout.start()
    dsts = (ko_ref, vo_ref)
    rd, wr = reads_and_writes((k_ref, v_ref), dsts, buf, isem, osem)
    order = [(t, i) for i in range(8) for t in range(2)]

    def inside(b):
        r = pos_ref[b] - base
        return r, (r >= 0) & (r < 64)

    @pl.when(early)
    def _():
        def row(t, b, r):
            return pltpu.make_async_copy(new_ref.at[t, b], dsts[t].at[b, r], rsem.at[t, b])

        for b in range(16):
            r, ok = inside(b)

            @pl.when(ok)
            def _():
                for t in range(2):
                    row(t, b, r).start()
        for b in range(16):
            r, ok = inside(b)

            @pl.when(ok)
            def _():
                for t in range(2):
                    row(t, b, r).wait()

    @pl.when(jnp.logical_not(early))
    def _():
        for t, i in order:
            rd(t, i).start()
        for t, i in order:
            rd(t, i).wait()
            for b in (2 * i, 2 * i + 1):
                r, ok = inside(b)

                @pl.when(ok)
                def _():
                    buf[t, b, r] = new_ref[t, b]
            wr(t, i).start()
        for t, i in order:
            wr(t, i).wait()

    yout.wait()


def solution(mesh):
    cache_spec = P('rep', 'seq', None, None)
    in_specs = (P('rep', None), P(), P(), P(), P('seq', None), cache_spec, cache_spec, P('rep'))
    out_specs = (P('rep', None), cache_spec, cache_spec)
    vmem, anyspace, smem = (pl.BlockSpec(memory_space=s) for s in (pltpu.VMEM, pl.ANY, pltpu.SMEM))
    dma = pltpu.SemaphoreType.DMA

    def local_step(x, wq, wk, wv, wo, k, v, pos):
        hbm = lambda *a: [pltpu.with_memory_space_constraint(t, pltpu.HBM) for t in a]
        cache = jax.ShapeDtypeStruct(k.shape, BF16)
        stage = [pltpu.VMEM((2, 16, 64, 8, 128), BF16), dma((2, 8)), dma((2, 8))]
        km, vm = pl.pallas_call(
            copy_kernel,
            name="copy_caches",
            out_shape=(cache, cache),
            in_specs=[anyspace] * 2,
            out_specs=(anyspace,) * 2,
            scratch_shapes=stage,
            compiler_params=pltpu.CompilerParams(vmem_limit_bytes=24 << 20),
        )(*hbm(k, v))
        x, km, vm = lax.optimization_barrier((x, km, vm))
        y, new = pl.pallas_call(
            main_kernel,
            name="decode",
            out_shape=(jax.ShapeDtypeStruct((2, 64, 8, 128), BF16),
                       jax.ShapeDtypeStruct((2, 2, 8, 8, 128), BF16)),
            in_specs=[anyspace] * 8,
            out_specs=(anyspace, vmem),
            scratch_shapes=[
                pltpu.SMEM((16,), jnp.int32), pltpu.VMEM((16, 8192), BF16),
                pltpu.VMEM((8, 512, 128), BF16), pltpu.VMEM((8, 512, 128), BF16),
                pltpu.VMEM((8192, 256), BF16), pltpu.VMEM((8192, 128), BF16),
                pltpu.VMEM((8, 2, 512, 128), BF16), pltpu.VMEM((8, 2, 512, 128), BF16),
                pltpu.VMEM((2, 64, 8192), BF16),
                pltpu.VMEM((2, 8, 256), BF16), pltpu.VMEM((32, 8, 256), BF16),
                pltpu.VMEM((2, 8, 128), BF16), pltpu.VMEM((16, 2, 8, 128), BF16),
                pltpu.VMEM((2, 2, 8, 8, 128), F32), pltpu.VMEM((8, 64, 128), F32),
                pltpu.VMEM((64, 1024), jnp.int32),
                pltpu.VMEM((64, 8, 128), F32), pltpu.VMEM((64, 8, 128), F32),
                pltpu.VMEM((64, 1, 128), F32), pltpu.VMEM((64, 1, 128), F32),
                pltpu.VMEM((64, 8, 128), F32), pltpu.VMEM((64, 8, 128), F32),
                pltpu.VMEM((8, 128), BF16), pltpu.VMEM((2, 64, 8, 128), BF16),
                dma((2,)), dma((2 * KCH,)), dma((5,)), dma((17,)), dma((17,)), dma((2,)), dma((2,)),
                dma, dma, dma, dma, dma, dma, dma, dma, dma, dma, dma, dma,
            ],
            compiler_params=pltpu.CompilerParams(collective_id=0, has_side_effects=True,
                                                 vmem_limit_bytes=DECODE_VMEM << 20),
        )(*hbm(pos, x, wq, wk, wv, wo, k.reshape(16, 512, 128), v.reshape(16, 512, 128)))
        yo, ko, vo = pl.pallas_call(
            update_kernel,
            name="update",
            out_shape=(jax.ShapeDtypeStruct(y.shape, BF16), cache, cache),
            in_specs=[smem, vmem, vmem] + [anyspace] * 4,
            out_specs=(anyspace,) * 3,
            scratch_shapes=[stage[0], dma, stage[1], stage[2], dma((2, 16))],
            input_output_aliases={5: 1, 6: 2},
            compiler_params=pltpu.CompilerParams(vmem_limit_bytes=24 << 20),
        )(pos, new.reshape(2, 16, 8, 128), y, *hbm(k, v, km, vm))
        return yo.transpose(0, 2, 1, 3).reshape(16, 8192), ko, vo

    return jax.shard_map(local_step, mesh=mesh, in_specs=in_specs, out_specs=out_specs, check_vma=False)
```

```python
import functools
import jax
import jax.numpy as jnp
from jax import lax
from jax.experimental import pallas as pl
from jax.experimental.pallas import tpu as pltpu
from jax.sharding import PartitionSpec as P

BF16 = jnp.bfloat16
F32 = jnp.float32
MESH = pl.DeviceIdType.MESH
DECODE_VMEM = 40
KCH = 8
RING = (0, 1, 2, 1)


def offsets():
    offs = [(dz, dy, dx) for dz in range(4) for dy in range(4) for dx in range(4)][1:]
    return sorted(offs, key=lambda o: -(RING[o[0]] + RING[o[1]] + RING[o[2]]))


def hops(o):
    return RING[o[0]] + RING[o[1]] + RING[o[2]]


def colour_offsets():
    best = {}
    for o in sorted(offsets(), key=lambda o: (hops(o), o)):
        d = ((o[2] + o[0]) % 4, (o[1] + o[0]) % 4)
        neg = ((-d[0]) % 4, (-d[1]) % 4)
        if d == (0, 0) or d in best or (d == neg and any(c % 2 for c in o)):
            continue
        best[d] = o
        best[neg] = tuple(-c % 4 for c in o)
    return sorted(best.values(), key=lambda o: -hops(o))


NEAR = [0, 1, 4]


def main_kernel(pos_hbm, x_hbm, wq_ref, wk_ref, wv_ref, wo_ref, k_ref, v_ref,
                y_ref, kvnew_ref, km_ref, vm_ref,
                pos_ref, x_ref, wqb, wkvb, kbuf, vbuf, wob, qsend, qrecv, kvsend, kvrecv, kvf, qf, colidx,
                opart, opeer, speer, oown, osend, orecv, ssend, srecv, ysend, yrecv, yb, yg,
                xsem, wsem, ksem, dw_send, dw_recv, d2d_send, d2d_recv, q_send, q_recv, o_send, o_recv,
                s_send, s_recv, ys_send, ys_recv, yg_send, yg_recv, pp_send, pp_recv, pn_send, pn_recv):
    me = lax.axis_index("seq")
    chip, core = me // 2, me % 2
    cx, cy, cz = chip % 4, (chip // 4) % 4, chip // 16
    other = 1 - core
    colour = ((cx + cz) % 4) * 4 + (cy + cz) % 4
    slot = colour * 2 + core

    def dev(d):
        return {"seq": d}

    def chip_at(o):
        return ((cz + o[0]) % 4) * 16 + ((cy + o[1]) % 4) * 4 + (cx + o[2]) % 4

    rows = 8192 // KCH
    qcol = pl.multiple_of(slot * 256, 256)
    kcol = pl.multiple_of((colour % 8) * 128, 128)

    def wq_copy(i):
        return pltpu.make_async_copy(wq_ref.at[pl.ds(i * rows, rows), pl.ds(qcol, 256)],
                                     wqb.at[pl.ds(i * rows, rows)], wsem.at[i])

    def wkv_copy(ref, i):
        return pltpu.make_async_copy(ref.at[pl.ds(i * rows, rows), pl.ds(kcol, 128)],
                                     wkvb.at[pl.ds(i * rows, rows)], wsem.at[KCH + i])

    xload = [pltpu.make_async_copy(x_hbm, x_ref, xsem.at[0]),
             pltpu.make_async_copy(pos_hbm, pos_ref, xsem.at[1])]
    for c in xload:
        c.start()
    for i in range(KCH):
        wq_copy(i).start()

    for ref, cond in ((wk_ref, colour < 8), (wv_ref, colour >= 8)):
        @pl.when((core == 1) & cond)
        def _():
            for i in range(KCH):
                wkv_copy(ref, i).start()

    loc = [pltpu.make_async_copy(k_ref, kbuf, ksem.at[0]),
           pltpu.make_async_copy(v_ref, vbuf, ksem.at[1]),
           pltpu.make_async_copy(wo_ref, wob.at[core], ksem.at[2]),
           pltpu.make_async_copy(k_ref, km_ref, ksem.at[3]),
           pltpu.make_async_copy(v_ref, vm_ref, ksem.at[4])]

    bar = pltpu.get_barrier_semaphore()
    partner = chip * 2 + other
    for o in offsets():
        pl.semaphore_signal(bar, inc=1, device_id=dev(chip_at(o) * 2 + core), device_id_type=MESH)
    for o in [(0, 0, 0)] + colour_offsets():
        pl.semaphore_signal(bar, inc=1, device_id=dev(chip_at(o) * 2 + other), device_id_type=MESH)
    near = functools.reduce(jnp.logical_or, [chip == c for c in NEAR])

    @pl.when(near)
    def _():
        for d in range(64):
            pl.semaphore_signal(bar, inc=1, device_id=dev(d * 2 + other), device_id_type=MESH)

    col = lax.broadcasted_iota(jnp.int32, (64, 512), 1)
    row = lax.broadcasted_iota(jnp.int32, (64, 512), 0)
    colidx[...] = jnp.where(col % 8 == row // 8, me * 64 + col // 8, 1 << 30)

    for c in xload:
        c.wait()
    accq = jnp.zeros((16, 256), F32)
    for i in range(KCH):
        wq_copy(i).wait()
        if i == KCH // 2:
            loc[0].start()
            loc[1].start()
        accq = accq + jnp.dot(x_ref[:, i * rows:(i + 1) * rows], wqb[i * rows:(i + 1) * rows, :],
                              preferred_element_type=F32)
    qsend[...] = accq.astype(BF16)
    loc[2].start()
    pl.semaphore_wait(bar, 79 + len(NEAR))

    def rcopy(src, dst, ss, rs, d):
        return pltpu.make_async_remote_copy(src_ref=src, dst_ref=dst, send_sem=ss, recv_sem=rs,
                                            device_id=dev(d), device_id_type=MESH)

    near_chips = [chip_at(o) for o in colour_offsets()]
    for ch in near_chips:
        for c2 in (core, other):
            rcopy(qsend, qrecv.at[slot], q_send.at[0], q_recv.at[0], ch * 2 + c2).start()
    rcopy(qsend, qrecv.at[slot], q_send.at[0], q_recv.at[0], partner).start()
    qrecv[slot] = qsend[...]

    @pl.when(core == 1)
    def _():
        acck = jnp.zeros((16, 128), F32)
        for i in range(KCH):
            wkv_copy(wk_ref, i).wait()
            acck = acck + jnp.dot(x_ref[:, i * rows:(i + 1) * rows], wkvb[i * rows:(i + 1) * rows, :],
                                  preferred_element_type=F32)
        for h in range(2):
            kvsend[h] = acck[h * 8:h * 8 + 8].astype(BF16)
        for ch in near_chips:
            for c2 in (core, other):
                rcopy(kvsend, kvrecv.at[colour], q_send.at[1], q_recv.at[1], ch * 2 + c2).start()
        rcopy(kvsend, kvrecv.at[colour], q_send.at[1], q_recv.at[1], partner).start()
        kvrecv[colour] = kvsend[...]

    def wait_all(ref, sem):
        pltpu.make_async_copy(ref, ref, sem).wait()

    wait_all(qrecv.at[pl.ds(0, 31)], q_recv.at[0])
    dw = rcopy(wo_ref, wob.at[core], dw_send, dw_recv, partner)
    dw.start()
    for s in range(32):
        q8 = qrecv[s].astype(F32)
        for j in range(2):
            qf[:, s * 2 + j, :] = q8[:, j * 128:(j + 1) * 128]

    @pl.when(core == 0)
    def _():
        wait_all(kvrecv.at[pl.ds(0, 16)], q_recv.at[1])

    @pl.when(core == 1)
    def _():
        wait_all(kvrecv.at[pl.ds(0, 15)], q_recv.at[1])

    for kv in range(2):
        for h in range(8):
            for half in range(2):
                kvf[kv, half, :, h, :] = kvrecv[kv * 8 + h, half].astype(F32)
    kvnew_ref[...] = kvf[...].astype(BF16)
    loc[0].wait()
    loc[1].wait()

    lane = lax.broadcasted_iota(jnp.int32, (64, 128), 1)
    scale = 128 ** -0.5
    neg = -jnp.inf

    def attend(half, dst):
        stats = jnp.zeros((64, 128), F32)
        for i in range(8):
            b = half * 8 + i
            pos = pos_ref[b]
            qb = qf[b]
            kn = jnp.broadcast_to(kvf[0, half, i][:, None, :], (8, 8, 128)).reshape(64, 128)
            vn = jnp.broadcast_to(kvf[1, half, i][:, None, :], (8, 8, 128)).reshape(64, 128)
            s = lax.dot_general(qb.astype(BF16), kbuf[b], (((1,), (1,)), ((), ())),
                                preferred_element_type=F32) * scale
            s = jnp.where(colidx[...] < pos, s, neg)
            snew = jnp.sum(qb * kn, axis=1, keepdims=True) * scale
            here = jnp.full((64, 1), pos // 64, jnp.int32) == me
            snew = jnp.where(here, snew, neg)
            m = jnp.maximum(jnp.max(s, axis=1, keepdims=True), snew)
            msafe = jnp.where(m == neg, 0.0, m)
            p = jnp.exp(s - msafe)
            pn = jnp.exp(snew - msafe)
            l = jnp.sum(p, axis=1, keepdims=True) + pn
            dst[i] = jnp.dot(p.astype(BF16), vbuf[b], preferred_element_type=F32) + pn * vn
            stats = jnp.where(lane == i, m, stats)
            stats = jnp.where(lane == 8 + i, l, stats)
        return stats

    ssend[:, 0, :] = attend(other, opart)
    do = [rcopy(opart, opeer, d2d_send.at[0], d2d_recv.at[0], partner),
          rcopy(ssend, speer, d2d_send.at[1], d2d_recv.at[1], partner)]
    for c in do:
        c.start()
    st1 = attend(core, oown)
    do[1].wait()
    st2 = speer[:, 0, :]
    do[0].wait()
    stats = jnp.zeros((64, 128), F32)
    for i in range(8):
        m1, m2 = st1[:, i:i + 1], st2[:, i:i + 1]
        l1, l2 = st1[:, 8 + i:9 + i], st2[:, 8 + i:9 + i]
        m = jnp.maximum(m1, m2)
        msafe = jnp.where(m == neg, 0.0, m)
        w1, w2 = jnp.exp(m1 - msafe), jnp.exp(m2 - msafe)
        osend[:, i, :] = w1 * oown[i] + w2 * opeer[i]
        stats = jnp.where(lane == i, m, stats)
        stats = jnp.where(lane == 8 + i, w1 * l1 + w2 * l2, stats)
    ssend[:, 0, :] = stats

    for o in offsets():
        d = chip_at(o)
        rcopy(osend.at[d], orecv.at[chip], o_send, o_recv, d * 2 + core).start()
        rcopy(ssend.at[d], srecv.at[chip], s_send, s_recv, d * 2 + core).start()
    loc[3].start()
    loc[4].start()
    orecv[chip] = osend[chip]
    srecv[chip] = ssend[chip]
    loc[2].wait()
    dw.wait_recv()
    wait_all(srecv.at[pl.ds(0, 63)], s_recv)
    st = jnp.concatenate([srecv[:, 0, :], jnp.zeros((64, 128), F32)], axis=0).T
    mt = st[0:8, 0:64]
    lt = st[8:16, 0:64]
    mx = jnp.max(mt, axis=1, keepdims=True)
    w = jnp.exp(mt - mx)
    tot = jnp.sum(w * lt, axis=1, keepdims=True)
    wait_all(orecv.at[pl.ds(0, 63)], o_recv)
    acc = jnp.zeros((8, 128), F32)
    for i in range(64):
        acc = acc + w[:, i:i + 1] * orecv[i]
    ob = (acc / tot).astype(BF16)

    pending = []
    for dz, dy in sorted([(a, b) for a in range(4) for b in range(4)], key=lambda o: -(RING[o[0]] + RING[o[1]])):
        r = ((cz + dz) % 4) * 4 + (cy + dy) % 4
        wj = wob[:, :, pl.ds(pl.multiple_of(r * 512, 512), 512)].reshape(128, 512)
        part = jnp.dot(ob, wj, preferred_element_type=F32)
        for jj in range(4):
            ysend[r * 4 + jj] = part[:, jj * 128:(jj + 1) * 128]
        for d in pending:
            rcopy(ysend.at[d], yrecv.at[chip], ys_send, ys_recv, d * 2 + core).start()
        pending = [chip_at((dz, dy, dx)) for dx in (2, 1, 3, 0) if (dz, dy, dx) != (0, 0, 0)]
    for d in pending:
        rcopy(ysend.at[d], yrecv.at[chip], ys_send, ys_recv, d * 2 + core).start()
    yrecv[chip] = ysend[chip]
    wait_all(yrecv.at[pl.ds(0, 63)], ys_recv)
    acc = yrecv[0]
    for i in range(1, 64):
        acc = acc + yrecv[i]
    yb[...] = acc.astype(BF16)

    for o in offsets():
        rcopy(yb, yg.at[core, chip], yg_send, yg_recv, chip_at(o) * 2 + core).start()
    for t in NEAR:
        rcopy(yb, yg.at[core, chip], pn_send, pn_recv, t * 2 + other).start()
    yg[core, chip] = yb[...]
    wait_all(yg.at[0, pl.ds(0, 63)], yg_recv)
    fwd = rcopy(yg.at[core], yg.at[core], pp_send, pp_recv, partner)

    @pl.when(near)
    def _():
        wait_all(yg.at[0], pn_recv)

    @pl.when(jnp.logical_not(near))
    def _():
        fwd.start()
        fwd.wait_recv()
        fwd.wait_send()

    out = pltpu.make_async_copy(yg, y_ref, ksem.at[0])
    out.start()

    wait_all(yg.at[0, pl.ds(0, 63)], yg_send)
    wait_all(yg.at[0, pl.ds(0, len(NEAR))], pn_send)
    wait_all(yrecv.at[pl.ds(0, 63)], ys_send)
    wait_all(orecv.at[pl.ds(0, 63)], o_send)
    wait_all(srecv.at[pl.ds(0, 63)], s_send)
    wait_all(qrecv.at[pl.ds(0, 31)], q_send.at[0])

    @pl.when(core == 1)
    def _():
        wait_all(kvrecv.at[pl.ds(0, 16)], q_send.at[1])
        wait_all(kvrecv.at[pl.ds(0, 15)], q_send.at[1])

    dw.wait_send()
    loc[3].wait()
    loc[4].wait()
    out.wait()


def update_kernel(pos_ref, new_ref, y_ref, k_ref, v_ref, yo_ref, ko_ref, vo_ref, patch, ysem, sem):
    base = lax.axis_index("seq") * 64
    yout = pltpu.make_async_copy(y_ref, yo_ref, ysem)
    yout.start()
    pairs = ((k_ref, ko_ref), (v_ref, vo_ref))
    for b in range(16):
        r = pos_ref[b] - base
        inside = (r >= 0) & (r < 64)
        for t, (src, dst) in enumerate(pairs):
            @pl.when(jnp.logical_not(inside))
            def _():
                pltpu.make_async_copy(src.at[b], dst.at[b], sem.at[t, b]).start()

            @pl.when(inside)
            def _():
                patch[t, b] = src[b]
                patch[t, b, r] = new_ref[t, b]
                pltpu.make_async_copy(patch.at[t, b], dst.at[b], sem.at[t, b]).start()
    for b in range(16):
        for t, (src, dst) in enumerate(pairs):
            pltpu.make_async_copy(patch.at[t, b], dst.at[b], sem.at[t, b]).wait()
    yout.wait()


def solution(mesh):
    cache_spec = P('rep', 'seq', None, None)
    in_specs = (P('rep', None), P(), P(), P(), P('seq', None), cache_spec, cache_spec, P('rep'))
    out_specs = (P('rep', None), cache_spec, cache_spec)
    vmem, anyspace, smem = (pl.BlockSpec(memory_space=s) for s in (pltpu.VMEM, pl.ANY, pltpu.SMEM))
    dma = pltpu.SemaphoreType.DMA

    def local_step(x, wq, wk, wv, wo, k, v, pos):
        hbm = lambda *a: [pltpu.with_memory_space_constraint(t, pltpu.HBM) for t in a]
        half = jax.ShapeDtypeStruct((16, 512, 128), BF16)
        y, new, km, vm = pl.pallas_call(
            main_kernel,
            name="decode",
            out_shape=(jax.ShapeDtypeStruct((2, 64, 8, 128), BF16),
                       jax.ShapeDtypeStruct((2, 2, 8, 8, 128), BF16), half, half),
            in_specs=[anyspace] * 8,
            out_specs=(anyspace, vmem, anyspace, anyspace),
            scratch_shapes=[
                pltpu.SMEM((16,), jnp.int32), pltpu.VMEM((16, 8192), BF16),
                pltpu.VMEM((8192, 256), BF16), pltpu.VMEM((8192, 128), BF16),
                pltpu.VMEM((16, 512, 128), BF16), pltpu.VMEM((16, 512, 128), BF16),
                pltpu.VMEM((2, 64, 8192), BF16),
                pltpu.VMEM((16, 256), BF16), pltpu.VMEM((32, 16, 256), BF16),
                pltpu.VMEM((2, 8, 128), BF16), pltpu.VMEM((16, 2, 8, 128), BF16),
                pltpu.VMEM((2, 2, 8, 8, 128), F32), pltpu.VMEM((16, 64, 128), F32),
                pltpu.VMEM((64, 512), jnp.int32),
                pltpu.VMEM((8, 64, 128), F32), pltpu.VMEM((8, 64, 128), F32),
                pltpu.VMEM((64, 1, 128), F32), pltpu.VMEM((8, 64, 128), F32),
                pltpu.VMEM((64, 8, 128), F32), pltpu.VMEM((64, 8, 128), F32),
                pltpu.VMEM((64, 1, 128), F32), pltpu.VMEM((64, 1, 128), F32),
                pltpu.VMEM((64, 8, 128), F32), pltpu.VMEM((64, 8, 128), F32),
                pltpu.VMEM((8, 128), BF16), pltpu.VMEM((2, 64, 8, 128), BF16),
                dma((2,)), dma((2 * KCH,)), dma((5,)), dma, dma, dma((2,)), dma((2,)), dma((2,)), dma((2,)),
                dma, dma, dma, dma, dma, dma, dma, dma, dma, dma, dma, dma,
            ],
            compiler_params=pltpu.CompilerParams(collective_id=0, has_side_effects=True,
                                                 vmem_limit_bytes=DECODE_VMEM << 20),
        )(*hbm(pos, x, wq, wk, wv, wo, k.reshape(16, 512, 128), v.reshape(16, 512, 128)))
        yo, ko, vo = pl.pallas_call(
            update_kernel,
            name="update",
            out_shape=(jax.ShapeDtypeStruct(y.shape, BF16),) + (jax.ShapeDtypeStruct(k.shape, BF16),) * 2,
            in_specs=[smem, vmem, vmem, vmem, vmem],
            out_specs=(anyspace,) * 3,
            scratch_shapes=[pltpu.VMEM((2, 16, 64, 8, 128), BF16), dma, dma((2, 16))],
            compiler_params=pltpu.CompilerParams(vmem_limit_bytes=24 << 20),
        )(pos, new.reshape(2, 16, 8, 128), y, km.reshape(k.shape), vm.reshape(k.shape))
        return yo.transpose(0, 2, 1, 3).reshape(16, 8192), ko, vo

    return jax.shard_map(local_step, mesh=mesh, in_specs=in_specs, out_specs=out_specs, check_vma=False)
```

```python
import functools
import jax
import jax.numpy as jnp
from jax import lax
from jax.experimental import pallas as pl
from jax.experimental.pallas import tpu as pltpu
from jax.sharding import PartitionSpec as P

BF16 = jnp.bfloat16
F32 = jnp.float32
MESH = pl.DeviceIdType.MESH
DECODE_VMEM = 40
KCH = 8
RING = (0, 1, 2, 1)


def offsets():
    offs = [(dz, dy, dx) for dz in range(4) for dy in range(4) for dx in range(4)][1:]
    return sorted(offs, key=lambda o: -(RING[o[0]] + RING[o[1]] + RING[o[2]]))


def hops(o):
    return RING[o[0]] + RING[o[1]] + RING[o[2]]


def colour_offsets():
    best = {}
    for o in sorted(offsets(), key=lambda o: (hops(o), o)):
        d = ((o[2] + o[0]) % 4, (o[1] + o[0]) % 4)
        neg = ((-d[0]) % 4, (-d[1]) % 4)
        if d == (0, 0) or d in best or (d == neg and any(c % 2 for c in o)):
            continue
        best[d] = o
        best[neg] = tuple(-c % 4 for c in o)
    return sorted(best.values(), key=lambda o: -hops(o))


NEAR = [0, 1, 4]


def main_kernel(pos_hbm, x_hbm, wq_ref, wk_ref, wv_ref, wo_ref, k_ref, v_ref,
                y_ref, kvnew_ref, km_ref, vm_ref,
                pos_ref, x_ref, wqb, wkvb, kbuf, vbuf, wob, qsend, qrecv, kvsend, kvrecv, kvf, qf, colidx,
                opart, opeer, speer, oown, osend, orecv, ssend, srecv, ysend, yrecv, yb, yg,
                ring_sem, xsem, wsem, ksem, dw_send, dw_recv, d2d_send, d2d_recv, q_send, q_recv, o_send, o_recv,
                s_send, s_recv, ys_send, ys_recv, yg_send, yg_recv, pp_send, pp_recv, pn_send, pn_recv):
    me = lax.axis_index("seq")
    chip, core = me // 2, me % 2
    cx, cy, cz = chip % 4, (chip // 4) % 4, chip // 16
    other = 1 - core
    colour = ((cx + cz) % 4) * 4 + (cy + cz) % 4
    slot = colour * 2 + core

    def dev(d):
        return {"seq": d}

    def chip_at(o):
        return ((cz + o[0]) % 4) * 16 + ((cy + o[1]) % 4) * 4 + (cx + o[2]) % 4

    rows = 8192 // KCH
    qcol = pl.multiple_of(slot * 256, 256)
    kcol = pl.multiple_of((colour % 8) * 128, 128)

    def wq_copy(i):
        return pltpu.make_async_copy(wq_ref.at[pl.ds(i * rows, rows), pl.ds(qcol, 256)],
                                     wqb.at[pl.ds(i * rows, rows)], wsem.at[i])

    def wkv_copy(ref, i):
        return pltpu.make_async_copy(ref.at[pl.ds(i * rows, rows), pl.ds(kcol, 128)],
                                     wkvb.at[pl.ds(i * rows, rows)], wsem.at[KCH + i])

    xload = [pltpu.make_async_copy(x_hbm, x_ref, xsem.at[0]),
             pltpu.make_async_copy(pos_hbm, pos_ref, xsem.at[1])]
    for c in xload:
        c.start()
    for i in range(KCH):
        wq_copy(i).start()

    for ref, cond in ((wk_ref, colour < 8), (wv_ref, colour >= 8)):
        @pl.when((core == 1) & cond)
        def _():
            for i in range(KCH):
                wkv_copy(ref, i).start()

    loc = [pltpu.make_async_copy(k_ref, kbuf, ksem.at[0]),
           pltpu.make_async_copy(v_ref, vbuf, ksem.at[1]),
           pltpu.make_async_copy(wo_ref, wob.at[core], ksem.at[2]),
           pltpu.make_async_copy(k_ref, km_ref, ksem.at[3]),
           pltpu.make_async_copy(v_ref, vm_ref, ksem.at[4])]

    bar = pltpu.get_barrier_semaphore()
    partner = chip * 2 + other
    near_chips = [chip_at(o) for o in colour_offsets()]
    for ch in near_chips:
        for c2 in (core, other):
            pl.semaphore_signal(bar, inc=1, device_id=dev(ch * 2 + c2), device_id_type=MESH)
    pl.semaphore_signal(bar, inc=1, device_id=dev(partner), device_id_type=MESH)
    near = functools.reduce(jnp.logical_or, [chip == c for c in NEAR])

    def greet(axis):
        for t in (2, 1, 3):
            o = [0, 0, 0]
            o[axis] = t
            pl.semaphore_signal(ring_sem.at[axis], inc=1, device_id=dev(chip_at(o) * 2 + core), device_id_type=MESH)

    def greeted(axis):
        pl.semaphore_wait(ring_sem.at[axis], 3)

    col = lax.broadcasted_iota(jnp.int32, (64, 512), 1)
    row = lax.broadcasted_iota(jnp.int32, (64, 512), 0)
    colidx[...] = jnp.where(col % 8 == row // 8, me * 64 + col // 8, 1 << 30)

    for c in xload:
        c.wait()
    accq = jnp.zeros((16, 256), F32)
    for i in range(KCH):
        wq_copy(i).wait()
        if i == KCH // 2:
            loc[0].start()
            loc[1].start()
        accq = accq + jnp.dot(x_ref[:, i * rows:(i + 1) * rows], wqb[i * rows:(i + 1) * rows, :],
                              preferred_element_type=F32)
    qsend[...] = accq.astype(BF16)
    loc[2].start()
    pl.semaphore_wait(bar, 31)
    greet(2)

    def rcopy(src, dst, ss, rs, d):
        return pltpu.make_async_remote_copy(src_ref=src, dst_ref=dst, send_sem=ss, recv_sem=rs,
                                            device_id=dev(d), device_id_type=MESH)

    for ch in near_chips:
        for c2 in (core, other):
            rcopy(qsend, qrecv.at[slot], q_send.at[0], q_recv.at[0], ch * 2 + c2).start()
    rcopy(qsend, qrecv.at[slot], q_send.at[0], q_recv.at[0], partner).start()
    qrecv[slot] = qsend[...]

    @pl.when(core == 1)
    def _():
        acck = jnp.zeros((16, 128), F32)
        for i in range(KCH):
            wkv_copy(wk_ref, i).wait()
            acck = acck + jnp.dot(x_ref[:, i * rows:(i + 1) * rows], wkvb[i * rows:(i + 1) * rows, :],
                                  preferred_element_type=F32)
        for h in range(2):
            kvsend[h] = acck[h * 8:h * 8 + 8].astype(BF16)
        for ch in near_chips:
            for c2 in (core, other):
                rcopy(kvsend, kvrecv.at[colour], q_send.at[1], q_recv.at[1], ch * 2 + c2).start()
        rcopy(kvsend, kvrecv.at[colour], q_send.at[1], q_recv.at[1], partner).start()
        kvrecv[colour] = kvsend[...]

    def wait_all(ref, sem):
        pltpu.make_async_copy(ref, ref, sem).wait()

    greeted(2)
    greet(1)
    greeted(1)
    greet(0)
    wait_all(qrecv.at[pl.ds(0, 31)], q_recv.at[0])
    dw = rcopy(wo_ref, wob.at[core], dw_send, dw_recv, partner)
    dw.start()
    for s in range(32):
        q8 = qrecv[s].astype(F32)
        for j in range(2):
            qf[:, s * 2 + j, :] = q8[:, j * 128:(j + 1) * 128]
    loc[0].wait()
    loc[1].wait()

    lane = lax.broadcasted_iota(jnp.int32, (64, 128), 1)
    scale = 128 ** -0.5
    neg = -jnp.inf

    def attend(half, dst):
        stats = jnp.zeros((64, 128), F32)
        for i in range(8):
            b = half * 8 + i
            pos = pos_ref[b]
            qb = qf[b]
            s = lax.dot_general(qb.astype(BF16), kbuf[b], (((1,), (1,)), ((), ())),
                                preferred_element_type=F32) * scale
            s = jnp.where(colidx[...] < pos, s, neg)
            m = jnp.max(s, axis=1, keepdims=True)
            p = jnp.exp(s - jnp.where(m == neg, 0.0, m))
            l = jnp.sum(p, axis=1, keepdims=True)
            dst[i] = jnp.dot(p.astype(BF16), vbuf[b], preferred_element_type=F32)
            stats = jnp.where(lane == i, m, stats)
            stats = jnp.where(lane == 8 + i, l, stats)
        return stats

    ssend[:, 0, :] = attend(other, opart)
    do = [rcopy(opart, opeer, d2d_send.at[0], d2d_recv.at[0], partner),
          rcopy(ssend, speer, d2d_send.at[1], d2d_recv.at[1], partner)]
    for c in do:
        c.start()
    st1 = attend(core, oown)

    @pl.when(core == 0)
    def _():
        wait_all(kvrecv.at[pl.ds(0, 16)], q_recv.at[1])

    @pl.when(core == 1)
    def _():
        wait_all(kvrecv.at[pl.ds(0, 15)], q_recv.at[1])

    for kv in range(2):
        for h in range(8):
            for half in range(2):
                kvf[kv, half, :, h, :] = kvrecv[kv * 8 + h, half].astype(F32)
    kvnew_ref[...] = kvf[...].astype(BF16)

    do[1].wait()
    st2 = speer[:, 0, :]
    do[0].wait()
    stats = jnp.zeros((64, 128), F32)
    for i in range(8):
        m1, m2 = st1[:, i:i + 1], st2[:, i:i + 1]
        l1, l2 = st1[:, 8 + i:9 + i], st2[:, 8 + i:9 + i]
        kn = jnp.broadcast_to(kvf[0, core, i][:, None, :], (8, 8, 128)).reshape(64, 128)
        vn = jnp.broadcast_to(kvf[1, core, i][:, None, :], (8, 8, 128)).reshape(64, 128)
        snew = jnp.sum(qf[core * 8 + i] * kn, axis=1, keepdims=True) * scale
        here = jnp.full((64, 1), pos_ref[core * 8 + i] // 128, jnp.int32) == chip
        snew = jnp.where(here, snew, neg)
        m = jnp.maximum(jnp.maximum(m1, m2), snew)
        msafe = jnp.where(m == neg, 0.0, m)
        w1, w2, w3 = jnp.exp(m1 - msafe), jnp.exp(m2 - msafe), jnp.exp(snew - msafe)
        osend[:, i, :] = w1 * oown[i] + w2 * opeer[i] + w3 * vn
        stats = jnp.where(lane == i, m, stats)
        stats = jnp.where(lane == 8 + i, w1 * l1 + w2 * l2 + w3, stats)
    ssend[:, 0, :] = stats

    greeted(0)

    for o in offsets():
        d = chip_at(o)
        rcopy(osend.at[d], orecv.at[chip], o_send, o_recv, d * 2 + core).start()
        rcopy(ssend.at[d], srecv.at[chip], s_send, s_recv, d * 2 + core).start()
    loc[3].start()
    loc[4].start()
    orecv[chip] = osend[chip]
    srecv[chip] = ssend[chip]
    loc[2].wait()
    dw.wait_recv()
    wait_all(srecv.at[pl.ds(0, 63)], s_recv)
    st = jnp.concatenate([srecv[:, 0, :], jnp.zeros((64, 128), F32)], axis=0).T
    mt = st[0:8, 0:64]
    lt = st[8:16, 0:64]
    mx = jnp.max(mt, axis=1, keepdims=True)
    w = jnp.exp(mt - mx)
    tot = jnp.sum(w * lt, axis=1, keepdims=True)
    wait_all(orecv.at[pl.ds(0, 63)], o_recv)
    acc = jnp.zeros((8, 128), F32)
    for i in range(64):
        acc = acc + w[:, i:i + 1] * orecv[i]
    ob = (acc / tot).astype(BF16)

    pending = []
    for dz, dy in sorted([(a, b) for a in range(4) for b in range(4)], key=lambda o: -(RING[o[0]] + RING[o[1]])):
        r = ((cz + dz) % 4) * 4 + (cy + dy) % 4
        wj = wob[:, :, pl.ds(pl.multiple_of(r * 512, 512), 512)].reshape(128, 512)
        part = jnp.dot(ob, wj, preferred_element_type=F32)
        for jj in range(4):
            ysend[r * 4 + jj] = part[:, jj * 128:(jj + 1) * 128]
        for d in pending:
            rcopy(ysend.at[d], yrecv.at[chip], ys_send, ys_recv, d * 2 + core).start()
        pending = [chip_at((dz, dy, dx)) for dx in (2, 1, 3, 0) if (dz, dy, dx) != (0, 0, 0)]
    for d in pending:
        rcopy(ysend.at[d], yrecv.at[chip], ys_send, ys_recv, d * 2 + core).start()
    yrecv[chip] = ysend[chip]
    wait_all(yrecv.at[pl.ds(0, 63)], ys_recv)
    acc = yrecv[0]
    for i in range(1, 64):
        acc = acc + yrecv[i]
    yb[...] = acc.astype(BF16)

    for o in offsets():
        rcopy(yb, yg.at[core, chip], yg_send, yg_recv, chip_at(o) * 2 + core).start()
    for t in NEAR:
        rcopy(yb, yg.at[core, chip], pn_send, pn_recv, t * 2 + other).start()
    yg[core, chip] = yb[...]
    wait_all(yg.at[0, pl.ds(0, 63)], yg_recv)
    fwd = rcopy(yg.at[core], yg.at[core], pp_send, pp_recv, partner)

    @pl.when(near)
    def _():
        wait_all(yg.at[0], pn_recv)

    @pl.when(jnp.logical_not(near))
    def _():
        fwd.start()
        fwd.wait_recv()
        fwd.wait_send()

    out = pltpu.make_async_copy(yg, y_ref, ksem.at[0])
    out.start()

    wait_all(yg.at[0, pl.ds(0, 63)], yg_send)
    wait_all(yg.at[0, pl.ds(0, len(NEAR))], pn_send)
    wait_all(yrecv.at[pl.ds(0, 63)], ys_send)
    wait_all(orecv.at[pl.ds(0, 63)], o_send)
    wait_all(srecv.at[pl.ds(0, 63)], s_send)
    wait_all(qrecv.at[pl.ds(0, 31)], q_send.at[0])

    @pl.when(core == 1)
    def _():
        wait_all(kvrecv.at[pl.ds(0, 16)], q_send.at[1])
        wait_all(kvrecv.at[pl.ds(0, 15)], q_send.at[1])

    dw.wait_send()
    loc[3].wait()
    loc[4].wait()
    out.wait()


def update_kernel(pos_ref, new_ref, y_ref, k_ref, v_ref, yo_ref, ko_ref, vo_ref, patch, ysem, sem):
    base = lax.axis_index("seq") * 64
    yout = pltpu.make_async_copy(y_ref, yo_ref, ysem)
    yout.start()
    pairs = ((k_ref, ko_ref), (v_ref, vo_ref))
    for b in range(16):
        r = pos_ref[b] - base
        inside = (r >= 0) & (r < 64)
        for t, (src, dst) in enumerate(pairs):
            @pl.when(jnp.logical_not(inside))
            def _():
                pltpu.make_async_copy(src.at[b], dst.at[b], sem.at[t, b]).start()

            @pl.when(inside)
            def _():
                patch[t, b] = src[b]
                patch[t, b, r] = new_ref[t, b]
                pltpu.make_async_copy(patch.at[t, b], dst.at[b], sem.at[t, b]).start()
    for b in range(16):
        for t, (src, dst) in enumerate(pairs):
            pltpu.make_async_copy(patch.at[t, b], dst.at[b], sem.at[t, b]).wait()
    yout.wait()


def solution(mesh):
    cache_spec = P('rep', 'seq', None, None)
    in_specs = (P('rep', None), P(), P(), P(), P('seq', None), cache_spec, cache_spec, P('rep'))
    out_specs = (P('rep', None), cache_spec, cache_spec)
    vmem, anyspace, smem = (pl.BlockSpec(memory_space=s) for s in (pltpu.VMEM, pl.ANY, pltpu.SMEM))
    dma = pltpu.SemaphoreType.DMA

    def local_step(x, wq, wk, wv, wo, k, v, pos):
        hbm = lambda *a: [pltpu.with_memory_space_constraint(t, pltpu.HBM) for t in a]
        half = jax.ShapeDtypeStruct((16, 512, 128), BF16)
        y, new, km, vm = pl.pallas_call(
            main_kernel,
            name="decode",
            out_shape=(jax.ShapeDtypeStruct((2, 64, 8, 128), BF16),
                       jax.ShapeDtypeStruct((2, 2, 8, 8, 128), BF16), half, half),
            in_specs=[anyspace] * 8,
            out_specs=(anyspace, vmem, anyspace, anyspace),
            scratch_shapes=[
                pltpu.SMEM((16,), jnp.int32), pltpu.VMEM((16, 8192), BF16),
                pltpu.VMEM((8192, 256), BF16), pltpu.VMEM((8192, 128), BF16),
                pltpu.VMEM((16, 512, 128), BF16), pltpu.VMEM((16, 512, 128), BF16),
                pltpu.VMEM((2, 64, 8192), BF16),
                pltpu.VMEM((16, 256), BF16), pltpu.VMEM((32, 16, 256), BF16),
                pltpu.VMEM((2, 8, 128), BF16), pltpu.VMEM((16, 2, 8, 128), BF16),
                pltpu.VMEM((2, 2, 8, 8, 128), F32), pltpu.VMEM((16, 64, 128), F32),
                pltpu.VMEM((64, 512), jnp.int32),
                pltpu.VMEM((8, 64, 128), F32), pltpu.VMEM((8, 64, 128), F32),
                pltpu.VMEM((64, 1, 128), F32), pltpu.VMEM((8, 64, 128), F32),
                pltpu.VMEM((64, 8, 128), F32), pltpu.VMEM((64, 8, 128), F32),
                pltpu.VMEM((64, 1, 128), F32), pltpu.VMEM((64, 1, 128), F32),
                pltpu.VMEM((64, 8, 128), F32), pltpu.VMEM((64, 8, 128), F32),
                pltpu.VMEM((8, 128), BF16), pltpu.VMEM((2, 64, 8, 128), BF16),
                pltpu.SemaphoreType.REGULAR((3,)), dma((2,)), dma((2 * KCH,)), dma((5,)), dma, dma, dma((2,)), dma((2,)), dma((2,)), dma((2,)),
                dma, dma, dma, dma, dma, dma, dma, dma, dma, dma, dma, dma,
            ],
            compiler_params=pltpu.CompilerParams(collective_id=0, has_side_effects=True,
                                                 vmem_limit_bytes=DECODE_VMEM << 20),
        )(*hbm(pos, x, wq, wk, wv, wo, k.reshape(16, 512, 128), v.reshape(16, 512, 128)))
        yo, ko, vo = pl.pallas_call(
            update_kernel,
            name="update",
            out_shape=(jax.ShapeDtypeStruct(y.shape, BF16),) + (jax.ShapeDtypeStruct(k.shape, BF16),) * 2,
            in_specs=[smem, vmem, vmem, vmem, vmem],
            out_specs=(anyspace,) * 3,
            scratch_shapes=[pltpu.VMEM((2, 16, 64, 8, 128), BF16), dma, dma((2, 16))],
            compiler_params=pltpu.CompilerParams(vmem_limit_bytes=24 << 20),
        )(pos, new.reshape(2, 16, 8, 128), y, km.reshape(k.shape), vm.reshape(k.shape))
        return yo.transpose(0, 2, 1, 3).reshape(16, 8192), ko, vo

    return jax.shard_map(local_step, mesh=mesh, in_specs=in_specs, out_specs=out_specs, check_vma=False)
```

```python
import functools
import jax
import jax.numpy as jnp
from jax import lax
from jax.experimental import pallas as pl
from jax.experimental.pallas import tpu as pltpu
from jax.sharding import PartitionSpec as P

BF16 = jnp.bfloat16
F32 = jnp.float32
MESH = pl.DeviceIdType.MESH
DECODE_VMEM = 40
LATE = 4
KCH = 8
RING = (0, 1, 2, 1)


def offsets():
    offs = [(dz, dy, dx) for dz in range(4) for dy in range(4) for dx in range(4)][1:]
    return sorted(offs, key=lambda o: -(RING[o[0]] + RING[o[1]] + RING[o[2]]))


def hops(o):
    return RING[o[0]] + RING[o[1]] + RING[o[2]]


def colour_offsets():
    best = {}
    for o in sorted(offsets(), key=lambda o: (hops(o), o)):
        d = ((o[2] + o[0]) % 4, (o[1] + o[0]) % 4)
        neg = ((-d[0]) % 4, (-d[1]) % 4)
        if d == (0, 0) or d in best or (d == neg and any(c % 2 for c in o)):
            continue
        best[d] = o
        best[neg] = tuple(-c % 4 for c in o)
    return sorted(best.values(), key=lambda o: -hops(o))


NEAR = [0, 1, 4]


def main_kernel(pos_hbm, x_hbm, wq_ref, wk_ref, wv_ref, wo_ref, k_ref, v_ref,
                y_ref, kvnew_ref, km_ref, vm_ref,
                pos_ref, x_ref, wqb, wkvb, kbuf, kt, vbuf, wob, qsend, qrecv, kvsend, kvrecv, kvf, qf, colidx,
                opart, opeer, speer, oown, osum, osend, orecv, ssend, srecv, ysend, yrecv, yb, yg,
                ring_sem, xsem, wsem, ksem, dw_send, dw_recv, d2d_send, d2d_recv, q_send, q_recv, o_send, o_recv,
                s_send, s_recv, ys_send, ys_recv, yg_send, yg_recv, pp_send, pp_recv, pn_send, pn_recv):
    me = lax.axis_index("seq")
    chip, core = me // 2, me % 2
    cx, cy, cz = chip % 4, (chip // 4) % 4, chip // 16
    other = 1 - core
    colour = ((cx + cz) % 4) * 4 + (cy + cz) % 4
    slot = colour * 2 + core

    def dev(d):
        return {"seq": d}

    zs, ys, xs = ([((c + i) % 4) * n for i in range(4)] for c, n in ((cz, 16), (cy, 4), (cx, 1)))

    def chip_at(o):
        return zs[o[0]] + ys[o[1]] + xs[o[2]]

    rows = 8192 // KCH
    qcol = pl.multiple_of(slot * 256, 256)
    kcol = pl.multiple_of((colour % 8) * 128, 128)

    def wq_copy(i):
        return pltpu.make_async_copy(wq_ref.at[pl.ds(i * rows, rows), pl.ds(qcol, 256)],
                                     wqb.at[pl.ds(i * rows, rows)], wsem.at[i])

    def wkv_copy(ref, i):
        return pltpu.make_async_copy(ref.at[pl.ds(i * rows, rows), pl.ds(kcol, 128)],
                                     wkvb.at[pl.ds(i * rows, rows)], wsem.at[KCH + i])

    xload = [pltpu.make_async_copy(x_hbm, x_ref, xsem.at[0]),
             pltpu.make_async_copy(pos_hbm, pos_ref, xsem.at[1])]
    for c in xload:
        c.start()
    for i in range(KCH):
        wq_copy(i).start()

    for ref, cond in ((wk_ref, colour < 8), (wv_ref, colour >= 8)):
        @pl.when((core == 1) & cond)
        def _():
            for i in range(KCH):
                wkv_copy(ref, i).start()

    loc = [pltpu.make_async_copy(k_ref, kbuf, ksem.at[0]),
           pltpu.make_async_copy(v_ref, vbuf, ksem.at[1]),
           pltpu.make_async_copy(wo_ref, wob.at[core], ksem.at[2]),
           pltpu.make_async_copy(k_ref, km_ref, ksem.at[3]),
           pltpu.make_async_copy(v_ref, vm_ref, ksem.at[4])]

    bar = pltpu.get_barrier_semaphore()
    partner = chip * 2 + other
    near_chips = [chip_at(o) for o in colour_offsets()]
    for ch in near_chips:
        for c2 in (core, other):
            pl.semaphore_signal(bar, inc=1, device_id=dev(ch * 2 + c2), device_id_type=MESH)
    pl.semaphore_signal(bar, inc=1, device_id=dev(partner), device_id_type=MESH)
    near = functools.reduce(jnp.logical_or, [chip == c for c in NEAR])

    def greet(axis):
        for t in (2, 1, 3):
            o = [0, 0, 0]
            o[axis] = t
            pl.semaphore_signal(ring_sem.at[axis], inc=1, device_id=dev(chip_at(o) * 2 + core), device_id_type=MESH)

    def greeted(axis):
        pl.semaphore_wait(ring_sem.at[axis], 3)

    col = lax.broadcasted_iota(jnp.int32, (64, 512), 1)
    row = lax.broadcasted_iota(jnp.int32, (64, 512), 0)
    colidx[...] = jnp.where(col % 8 == row // 8, me * 64 + col // 8, 1 << 30)

    for c in xload:
        c.wait()
    accq = jnp.zeros((16, 256), F32)
    for i in range(KCH):
        wq_copy(i).wait()
        if i == KCH // 2:
            loc[0].start()
            loc[1].start()
        accq = accq + jnp.dot(x_ref[:, i * rows:(i + 1) * rows], wqb[i * rows:(i + 1) * rows, :],
                              preferred_element_type=F32)
    for h in range(2):
        qsend[h] = accq[h * 8:h * 8 + 8].astype(BF16)
    loc[2].start()
    pl.semaphore_wait(bar, 31)
    greet(2)

    def rcopy(src, dst, ss, rs, d):
        return pltpu.make_async_remote_copy(src_ref=src, dst_ref=dst, send_sem=ss, recv_sem=rs,
                                            device_id=dev(d), device_id_type=MESH)

    for ch in near_chips:
        for c2 in (core, other):
            rcopy(qsend, qrecv.at[slot], q_send.at[0], q_recv.at[0], ch * 2 + c2).start()
    rcopy(qsend, qrecv.at[slot], q_send.at[0], q_recv.at[0], partner).start()
    qrecv[slot] = qsend[...]

    @pl.when(core == 1)
    def _():
        acck = jnp.zeros((16, 128), F32)
        for i in range(KCH):
            wkv_copy(wk_ref, i).wait()
            acck = acck + jnp.dot(x_ref[:, i * rows:(i + 1) * rows], wkvb[i * rows:(i + 1) * rows, :],
                                  preferred_element_type=F32)
        for h in range(2):
            kvsend[h] = acck[h * 8:h * 8 + 8].astype(BF16)
        for ch in near_chips:
            for c2 in (core, other):
                rcopy(kvsend, kvrecv.at[colour], q_send.at[1], q_recv.at[1], ch * 2 + c2).start()
        rcopy(kvsend, kvrecv.at[colour], q_send.at[1], q_recv.at[1], partner).start()
        kvrecv[colour] = kvsend[...]

    def wait_all(ref, sem):
        pltpu.make_async_copy(ref, ref, sem).wait()

    greeted(2)
    greet(1)
    loc[0].wait()
    for b in range(16):
        kt[b] = kbuf[b].T
    greeted(1)
    greet(0)
    wait_all(qrecv.at[pl.ds(0, 31)], q_recv.at[0])
    dw = rcopy(wo_ref, wob.at[core], dw_send, dw_recv, partner)
    dw.start()

    def spread_q(half):
        for s in range(32):
            q8 = qrecv[s, half].astype(F32)
            for j in range(2):
                qf[half, pl.ds((s * 2 + j) * 8, 8), :] = q8[:, j * 128:(j + 1) * 128]

    loc[1].wait()
    lane = lax.broadcasted_iota(jnp.int32, (64, 128), 1)
    scale = 128 ** -0.5
    neg = -jnp.inf

    def attend(half, dst, mst, lst, which):
        for i in which:
            b = half * 8 + i
            pos = pos_ref[b]
            qb = qf[half, pl.ds(i, 64, stride=8), :]
            s = jnp.dot(qb.astype(BF16), kt[b], preferred_element_type=F32) * scale
            s = jnp.where(colidx[...] < pos, s, neg)
            m = jnp.max(s, axis=1, keepdims=True)
            p = jnp.exp(s - jnp.where(m == neg, 0.0, m))
            l = jnp.sum(p, axis=1, keepdims=True)
            dst[i] = jnp.dot(p.astype(BF16), vbuf[b], preferred_element_type=F32)
            mst = jnp.where(lane == i, m, mst)
            lst = jnp.where(lane == i, l, lst)
        return mst, lst

    def pack(m, l):
        return jnp.where(lane < 8, m, pltpu.roll(l, 8, 1))

    spread_q(other)
    none = jnp.zeros((64, 128), F32)
    ssend[:, 0, :] = pack(*attend(other, opart, none, none, range(8)))
    spread_q(core)
    do = [rcopy(opart, opeer, d2d_send.at[0], d2d_recv.at[0], partner),
          rcopy(ssend, speer, d2d_send.at[1], d2d_recv.at[1], partner)]
    for c in do:
        c.start()
    m1, l1 = attend(core, oown, none, none, range(LATE))

    @pl.when(core == 0)
    def _():
        wait_all(kvrecv.at[pl.ds(0, 16)], q_recv.at[1])

    @pl.when(core == 1)
    def _():
        wait_all(kvrecv.at[pl.ds(0, 15)], q_recv.at[1])

    for kv in range(2):
        for h in range(8):
            for half in range(2):
                kvf[kv, half, :, h, :] = kvrecv[kv * 8 + h, half].astype(F32)
    kvnew_ref[...] = kvf[...].astype(BF16)

    do[1].wait()
    st2 = speer[:, 0, :]
    do[0].wait()
    m1, l1 = attend(core, oown, m1, l1, range(LATE, 8))
    m2, l2, m3 = st2, pltpu.roll(st2, 120, 1), none
    for i in range(8):
        kn = jnp.broadcast_to(kvf[0, core, i][:, None, :], (8, 8, 128)).reshape(64, 128)
        snew = jnp.sum(qf[core, pl.ds(i, 64, stride=8), :] * kn, axis=1, keepdims=True) * scale
        here = jnp.full((64, 1), pos_ref[core * 8 + i] // 128, jnp.int32) == chip
        m3 = jnp.where(lane == i, jnp.where(here, snew, neg), m3)
    m = jnp.maximum(jnp.maximum(m1, m2), m3)
    msafe = jnp.where(m == neg, 0.0, m)
    w1, w2, w3 = jnp.exp(m1 - msafe), jnp.exp(m2 - msafe), jnp.exp(m3 - msafe)
    stats = pack(m, w1 * l1 + w2 * l2 + w3)
    for i in range(8):
        vn = jnp.broadcast_to(kvf[1, core, i][:, None, :], (8, 8, 128)).reshape(64, 128)
        osum[pl.ds(i * 64, 64), :] = (w1[:, i:i + 1] * oown[i] + w2[:, i:i + 1] * opeer[i] + w3[:, i:i + 1] * vn)
    ssend[:, 0, :] = stats
    for h in range(64):
        osend[h] = osum[pl.ds(h, 8, stride=64), :]

    greeted(0)

    for o in offsets():
        d = chip_at(o)
        rcopy(osend.at[d], orecv.at[chip], o_send, o_recv, d * 2 + core).start()
        rcopy(ssend.at[d], srecv.at[chip], s_send, s_recv, d * 2 + core).start()
    loc[3].start()
    loc[4].start()
    orecv[chip] = osend[chip]
    srecv[chip] = ssend[chip]
    loc[2].wait()
    dw.wait_recv()
    wait_all(srecv.at[pl.ds(0, 63)], s_recv)
    st = jnp.concatenate([srecv[:, 0, :], jnp.zeros((64, 128), F32)], axis=0).T
    mt = st[0:8, 0:64]
    lt = st[8:16, 0:64]
    mx = jnp.max(mt, axis=1, keepdims=True)
    w = jnp.exp(mt - mx)
    tot = jnp.sum(w * lt, axis=1, keepdims=True)
    wait_all(orecv.at[pl.ds(0, 63)], o_recv)
    acc = jnp.zeros((8, 128), F32)
    for i in range(64):
        acc = acc + w[:, i:i + 1] * orecv[i]
    ob = (acc / tot).astype(BF16)

    pending = []
    for dz, dy in sorted([(a, b) for a in range(4) for b in range(4)], key=lambda o: -(RING[o[0]] + RING[o[1]])):
        r = ((cz + dz) % 4) * 4 + (cy + dy) % 4
        wj = wob[:, :, pl.ds(pl.multiple_of(r * 512, 512), 512)].reshape(128, 512)
        part = jnp.dot(ob, wj, preferred_element_type=F32)
        for jj in range(4):
            ysend[r * 4 + jj] = part[:, jj * 128:(jj + 1) * 128]
        for d in pending:
            rcopy(ysend.at[d], yrecv.at[chip], ys_send, ys_recv, d * 2 + core).start()
        pending = [chip_at((dz, dy, dx)) for dx in (2, 1, 3, 0) if (dz, dy, dx) != (0, 0, 0)]
    for d in pending:
        rcopy(ysend.at[d], yrecv.at[chip], ys_send, ys_recv, d * 2 + core).start()
    yrecv[chip] = ysend[chip]
    wait_all(yrecv.at[pl.ds(0, 63)], ys_recv)
    acc = yrecv[0]
    for i in range(1, 64):
        acc = acc + yrecv[i]
    yb[...] = acc.astype(BF16)

    for o in offsets():
        rcopy(yb, yg.at[core, chip], yg_send, yg_recv, chip_at(o) * 2 + core).start()
    for t in NEAR:
        rcopy(yb, yg.at[core, chip], pn_send, pn_recv, t * 2 + other).start()
    yg[core, chip] = yb[...]
    wait_all(yg.at[0, pl.ds(0, 63)], yg_recv)
    fwd = rcopy(yg.at[core], yg.at[core], pp_send, pp_recv, partner)

    @pl.when(near)
    def _():
        wait_all(yg.at[0], pn_recv)

    @pl.when(jnp.logical_not(near))
    def _():
        fwd.start()
        fwd.wait_recv()
        fwd.wait_send()

    out = pltpu.make_async_copy(yg, y_ref, ksem.at[0])
    out.start()

    wait_all(yg.at[0, pl.ds(0, 63)], yg_send)
    wait_all(yg.at[0, pl.ds(0, len(NEAR))], pn_send)
    wait_all(yrecv.at[pl.ds(0, 63)], ys_send)
    wait_all(orecv.at[pl.ds(0, 63)], o_send)
    wait_all(srecv.at[pl.ds(0, 63)], s_send)
    wait_all(qrecv.at[pl.ds(0, 31)], q_send.at[0])

    @pl.when(core == 1)
    def _():
        wait_all(kvrecv.at[pl.ds(0, 16)], q_send.at[1])
        wait_all(kvrecv.at[pl.ds(0, 15)], q_send.at[1])

    dw.wait_send()
    loc[3].wait()
    loc[4].wait()
    out.wait()


def update_kernel(pos_ref, new_ref, y_ref, k_ref, v_ref, yo_ref, ko_ref, vo_ref, patch, ysem, sem):
    base = lax.axis_index("seq") * 64
    yout = pltpu.make_async_copy(y_ref, yo_ref, ysem)
    yout.start()
    pairs = ((k_ref, ko_ref), (v_ref, vo_ref))
    for b in range(16):
        r = pos_ref[b] - base
        inside = (r >= 0) & (r < 64)
        for t, (src, dst) in enumerate(pairs):
            @pl.when(jnp.logical_not(inside))
            def _():
                pltpu.make_async_copy(src.at[b], dst.at[b], sem.at[t, b]).start()

            @pl.when(inside)
            def _():
                patch[t, b] = src[b]
                patch[t, b, r] = new_ref[t, b]
                pltpu.make_async_copy(patch.at[t, b], dst.at[b], sem.at[t, b]).start()
    for b in range(16):
        for t, (src, dst) in enumerate(pairs):
            pltpu.make_async_copy(patch.at[t, b], dst.at[b], sem.at[t, b]).wait()
    yout.wait()


def solution(mesh):
    cache_spec = P('rep', 'seq', None, None)
    in_specs = (P('rep', None), P(), P(), P(), P('seq', None), cache_spec, cache_spec, P('rep'))
    out_specs = (P('rep', None), cache_spec, cache_spec)
    vmem, anyspace, smem = (pl.BlockSpec(memory_space=s) for s in (pltpu.VMEM, pl.ANY, pltpu.SMEM))
    dma = pltpu.SemaphoreType.DMA

    def local_step(x, wq, wk, wv, wo, k, v, pos):
        hbm = lambda *a: [pltpu.with_memory_space_constraint(t, pltpu.HBM) for t in a]
        half = jax.ShapeDtypeStruct((16, 512, 128), BF16)
        y, new, km, vm = pl.pallas_call(
            main_kernel,
            name="decode",
            out_shape=(jax.ShapeDtypeStruct((2, 64, 8, 128), BF16),
                       jax.ShapeDtypeStruct((2, 2, 8, 8, 128), BF16), half, half),
            in_specs=[anyspace] * 8,
            out_specs=(anyspace, vmem, anyspace, anyspace),
            scratch_shapes=[
                pltpu.SMEM((16,), jnp.int32), pltpu.VMEM((16, 8192), BF16),
                pltpu.VMEM((8192, 256), BF16), pltpu.VMEM((8192, 128), BF16),
                pltpu.VMEM((16, 512, 128), BF16), pltpu.VMEM((16, 128, 512), BF16),
                pltpu.VMEM((16, 512, 128), BF16), pltpu.VMEM((2, 64, 8192), BF16),
                pltpu.VMEM((2, 8, 256), BF16), pltpu.VMEM((32, 2, 8, 256), BF16),
                pltpu.VMEM((2, 8, 128), BF16), pltpu.VMEM((16, 2, 8, 128), BF16),
                pltpu.VMEM((2, 2, 8, 8, 128), F32), pltpu.VMEM((2, 512, 128), F32),
                pltpu.VMEM((64, 512), jnp.int32),
                pltpu.VMEM((8, 64, 128), F32), pltpu.VMEM((8, 64, 128), F32),
                pltpu.VMEM((64, 1, 128), F32), pltpu.VMEM((8, 64, 128), F32), pltpu.VMEM((512, 128), F32),
                pltpu.VMEM((64, 8, 128), F32), pltpu.VMEM((64, 8, 128), F32),
                pltpu.VMEM((64, 1, 128), F32), pltpu.VMEM((64, 1, 128), F32),
                pltpu.VMEM((64, 8, 128), F32), pltpu.VMEM((64, 8, 128), F32),
                pltpu.VMEM((8, 128), BF16), pltpu.VMEM((2, 64, 8, 128), BF16),
                pltpu.SemaphoreType.REGULAR((3,)), dma((2,)), dma((2 * KCH,)), dma((5,)), dma, dma, dma((2,)), dma((2,)), dma((2,)), dma((2,)),
                dma, dma, dma, dma, dma, dma, dma, dma, dma, dma, dma, dma,
            ],
            compiler_params=pltpu.CompilerParams(collective_id=0, has_side_effects=True,
                                                 vmem_limit_bytes=DECODE_VMEM << 20),
        )(*hbm(pos, x, wq, wk, wv, wo, k.reshape(16, 512, 128), v.reshape(16, 512, 128)))
        yo, ko, vo = pl.pallas_call(
            update_kernel,
            name="update",
            out_shape=(jax.ShapeDtypeStruct(y.shape, BF16),) + (jax.ShapeDtypeStruct(k.shape, BF16),) * 2,
            in_specs=[smem, vmem, vmem, vmem, vmem],
            out_specs=(anyspace,) * 3,
            scratch_shapes=[pltpu.VMEM((2, 16, 64, 8, 128), BF16), dma, dma((2, 16))],
            compiler_params=pltpu.CompilerParams(vmem_limit_bytes=24 << 20),
        )(pos, new.reshape(2, 16, 8, 128), y, km.reshape(k.shape), vm.reshape(k.shape))
        return yo.transpose(0, 2, 1, 3).reshape(16, 8192), ko, vo

    return jax.shard_map(local_step, mesh=mesh, in_specs=in_specs, out_specs=out_specs, check_vma=False)
```
